32 devices in a mesh: ctx: 4 (over x, core), exp: 8 (over z, y).
Axes of the slice: x: 2, y: 2, z: 4, core: 2. Of those that a mesh axis runs over, the one named last changes fastest.
Arguments:
- q_nope: bfloat16 [128, 128, 512], P('ctx', 'exp'), may hold values from -72 to 72
- q_rope: bfloat16 [128, 8192], P('ctx', 'exp'), may hold values from -6 to 6
- cache_keys: bfloat16 [576, 512], P(None, 'ctx'), may hold values from -6 to 6
- fresh_keys: bfloat16 [576, 128], P(None, 'ctx'), may hold values from -6 to 6
- block_order: int32 [8], replicated, may hold values from 0 to 7, each once
- w_uv: bfloat16 [128, 512, 128], P('exp'), may hold values from -0.25 to 0.25
- w_out: bfloat16 [16384, 7168], P('exp', 'ctx'), may hold values from -0.046875 to 0.046875
- residual: bfloat16 [128, 7168], P(('ctx', 'exp')), may hold values from -6 to 6
- norm_gain: float32 [7168], replicated, may hold values from 0.5 to 1.5
- router_weight: bfloat16 [7168, 16], replicated, may hold values from -0.0625 to 0.0625
- expert_ids: int32 [128, 8], P(('ctx', 'exp')), may hold values from 0 to 15, all different within a row; in each aligned block of 4 rows (0 to 3, 4 to 7, ...) at most 3 rows name the same one
- w_gate: bfloat16 [16, 7168, 2048], P('exp', None, 'ctx'), may hold values from -0.0625 to 0.0625
- w_up: bfloat16 [16, 7168, 2048], P('exp', None, 'ctx'), may hold values from -0.0625 to 0.0625
- w_down: bfloat16 [16, 2048, 7168], P('exp', 'ctx'), may hold values from -0.125 to 0.125
Outputs:
- layer_out: bfloat16 [128, 7168], P(('ctx', 'exp'))
The draws below stay inside these ranges and needn't reach their ends.
Inputs may be any that keep to these rules, and one draw needn't show every extreme that they name: A permutation: block j of the new tokens (16 rows) sits at positions 512 + block_order[j] * 16 onward. `expert_ids`: each row names 8 different experts; the 4 rows of one device name no expert more than 3 times, and in some aligned block one expert exactly 3 times.
All inputs are finite; a program needn't handle non-finite values.
Results may differ from the reference program's by a relative error of at most 0.012.
Values may be sent and summed in bfloat16 or wider, within the bound.
A program may use at most 128 MiB of HBM per device.

```python
import math
import jax
import jax.numpy as jnp
import numpy as np
from jax import lax

D = 7168
HEADS = 128
LAT = 512
ROPE = 64
QKD = 192
VHD = 128
FF = 2048
TOP = 8
EXPERTS = 16
TOK_DEV = 4
KD = 576
FFS = 512
CAP = 3
BLK = 16
NBLK = 8
NEWTOK = 128
CACHE = 512


def latent_cache(key):
    baseline = jax.random.normal(jax.random.fold_in(key, 101), (KD, CACHE), jnp.float32)
    return jnp.clip(baseline, -6.0, 6.0)


def draw_cache_keys(key, part):
    return latent_cache(key).astype(jnp.bfloat16)


def draw_q_nope(key, part):
    queries = jnp.clip(jax.random.normal(jax.random.fold_in(key, 202), (NEWTOK, HEADS, LAT), jnp.float32), -6.0, 6.0)
    return queries.astype(jnp.bfloat16)


def steps_of(rng, dims, cuts, low, top_value):
    loudness = 1.0
    for position, parts in cuts:
        steps = jax.random.uniform(jax.random.fold_in(jax.random.fold_in(rng, 6), position), (parts,), jnp.float32, low / len(cuts), top_value / len(cuts))
        loudness = loudness * jnp.repeat(jnp.exp(steps), dims[position] // parts).reshape((-1,) + (1,) * (len(dims) - 1 - position))
    return loudness


def shared_out(own_key, own, number, rows, amount, top, limit, skew):
    sequence = jax.random.permutation(own_key, amount)
    crowded, common = load_shares(amount, rows * top, limit, skew, True), load_shares(amount, rows * top, limit, skew, False)
    places = jnp.arange(amount)

    def named(tallies, rotation):
        used = int((tallies > 0).sum())
        fixed = max(1, used // 4)
        moved = fixed + (places - fixed + rotation * (used - fixed)) % max(1, amount - fixed)
        return jnp.zeros((amount,), jnp.int32).at[sequence[jnp.where(places < fixed, places, moved)]].set(jnp.asarray(tallies, jnp.int32))

    tallies = jnp.where(number % 4 == 0, named(crowded, number // 4), named(common, number - number // 4 - 1))
    mixed = jax.random.permutation(jax.random.fold_in(own, 3), amount)
    source_of, sink = mixed[0:amount // 2 * 2:2], mixed[1:amount // 2 * 2:2]
    room = jnp.minimum(tallies[source_of] - 1, limit - tallies[sink]) // 2
    room = jnp.where((source_of == sequence[0]) | (sink == sequence[0]) | (tallies[sink] == 0), 0, jnp.maximum(room, 0))
    moved = jax.random.randint(jax.random.fold_in(own, 4), (amount // 2,), 0, 1 << 20) % (room + 1)
    tallies = tallies.at[source_of].add(-moved).at[sink].add(moved)
    items = jnp.searchsorted(jnp.cumsum(tallies), jnp.arange(rows * top), side="right").astype(jnp.int32)
    table = items.reshape(top, rows).T
    table = table[jax.random.permutation(jax.random.fold_in(own, 1), rows)]
    rotation = jax.random.randint(jax.random.fold_in(own, 2), (rows, 1), 0, top)
    return jnp.take_along_axis(table, (jnp.arange(top)[None, :] + rotation) % top, axis=1)


def load_shares(count, total, bound, slope, full):
    loads = [(1 << 20) // math.isqrt(grade ** slope) + 1 for grade in range(1, count + 1)]
    largest = bound if full else min(bound, max(-(-total // count), total * loads[0] // sum(loads)))
    least = 1 if total - largest >= count - 1 else 0
    given, spare = [largest] + [least] * (count - 1), total - largest - least * (count - 1)
    while spare > 0:
        candidates = [i for i in range(1, count) if given[i] < largest] or [i for i in range(1, count) if given[i] < bound]
        pool, remaining = sum([loads[i] for i in candidates]), spare
        for i in candidates:
            extra = min(bound - given[i], max(1, remaining * loads[i] // pool), spare)
            given[i] = given[i] + extra
            spare = spare - extra
    return np.array(given)


def centred(stream_key, dims, width, most, cuts=(), kind=jnp.bfloat16):
    values = jax.random.normal(stream_key, dims, jnp.float32) * width
    if len(cuts) > 0:
        values = steps_of(stream_key, dims, cuts, -0.22, 0.18) * values
    return jnp.clip(values, min=-most, max=most).astype(kind)


def setup_inputs(seed: int = 0) -> dict:
    key_of = jax.random.split(jax.random.key(seed), 15)
    q_nope = draw_q_nope(jax.random.fold_in(key_of[14], 71), 0)
    q_rope = centred(key_of[1], (NEWTOK, HEADS * ROPE), 1.0, 6.0, ((0, 4), (1, 8)))
    cache_keys = draw_cache_keys(jax.random.fold_in(key_of[14], 71), 0)
    fresh_keys = centred(key_of[3], (KD, NEWTOK), 1.0, 6.0, ((1, 4),))
    block_order = jax.random.permutation(key_of[4], NBLK).astype(jnp.int32)
    w_uv = centred(key_of[5], (HEADS, LAT, VHD), LAT ** -0.5, 0.25, ((0, 8),))
    w_out = centred(key_of[6], (HEADS * VHD, D), (HEADS * VHD) ** -0.5, 0.046875, ((0, 8), (1, 4)))
    residual = centred(key_of[7], (NEWTOK, D), 1.0, 6.0, ((0, 32),))
    norm_gain = jnp.clip(1.0 + 0.1 * jax.random.normal(key_of[8], (D,), jnp.float32), 0.5, 1.5)
    router_weight = centred(key_of[9], (D, EXPERTS), D ** -0.5, 0.0625)
    expert_ids_keys = jax.random.split(jax.random.fold_in(key_of[10], 1), NEWTOK // TOK_DEV)
    expert_ids_turns = jax.random.permutation(jax.random.fold_in(key_of[10], 3), NEWTOK // TOK_DEV)
    expert_ids = jax.vmap(lambda own, number: shared_out(jax.random.fold_in(key_of[10], 2), own, number, TOK_DEV, EXPERTS, TOP, CAP, 2))(expert_ids_keys, expert_ids_turns).reshape((NEWTOK, TOP))
    w_gate = centred(key_of[11], (EXPERTS, D, FF), D ** -0.5, 0.0625, ((0, 8), (2, 4)))
    w_up = centred(key_of[12], (EXPERTS, D, FF), D ** -0.5, 0.0625, ((0, 8), (2, 4)))
    w_down = centred(key_of[13], (EXPERTS, FF, D), FF ** -0.5, 0.125, ((0, 8), (1, 4)))
    return dict(q_nope=q_nope, q_rope=q_rope, cache_keys=cache_keys, fresh_keys=fresh_keys, block_order=block_order, w_uv=w_uv, w_out=w_out, residual=residual, norm_gain=norm_gain, router_weight=router_weight, expert_ids=expert_ids, w_gate=w_gate, w_up=w_up, w_down=w_down)


ROUTE_SCALE = 2.5
NORM_EPS = 1e-06

def block_position(row_index, block_order):
    blocks = row_index // BLK
    lookup = blocks[:, None] == jnp.arange(NBLK, dtype=jnp.int32)[None, :]
    leading = lax.optimization_barrier(jnp.sum(jnp.where(lookup, block_order[None, :], 0), axis=1))
    return (leading * BLK + row_index % BLK).astype(jnp.int32)

def reference(q_nope, q_rope, cache_keys, fresh_keys, block_order, w_uv, w_out, residual, norm_gain, router_weight, expert_ids, w_gate, w_up, w_down):
    keys = jnp.concatenate([cache_keys, fresh_keys], axis=1)
    query_pos = block_position(jnp.arange(NEWTOK, dtype=jnp.int32), block_order)
    key_pos = jnp.concatenate([jnp.full((CACHE,), -1, jnp.int32), query_pos])
    visible = key_pos[None, :] <= query_pos[:, None]
    scale = 1.0 / math.sqrt(QKD)
    latent_keys = keys[:LAT]
    rotary_keys = keys[LAT:]

    def one_head(inputs):
        query_lat, query_pe, w_head = inputs
        first_dot = jnp.dot(query_lat, latent_keys, preferred_element_type=jnp.float32)
        second_dot = jnp.dot(query_pe, rotary_keys, preferred_element_type=jnp.float32)
        scores = jnp.where(visible, (first_dot + second_dot) * scale, -jnp.inf)
        row_max = lax.optimization_barrier(jnp.max(scores, axis=1, keepdims=True))
        exponent = jnp.exp(scores - row_max)
        row_sum = lax.optimization_barrier(jnp.sum(exponent, axis=1, keepdims=True))
        latent = lax.dot_general(exponent.astype(jnp.bfloat16), latent_keys, (((1,), (1,)), ((), ())), preferred_element_type=jnp.float32) / row_sum
        return jnp.dot(latent, w_head.astype(jnp.float32), precision=lax.Precision.HIGHEST).astype(jnp.bfloat16)
    head_inputs = (jnp.transpose(q_nope, (1, 0, 2)), jnp.transpose(q_rope.reshape(NEWTOK, HEADS, ROPE), (1, 0, 2)), w_uv)
    head_out = lax.map(one_head, head_inputs)
    head_out = jnp.transpose(head_out, (1, 0, 2)).reshape(NEWTOK, HEADS * VHD)
    attention = jnp.dot(head_out, w_out, preferred_element_type=jnp.float32).astype(jnp.bfloat16)
    hidden = residual.astype(jnp.float32) + attention.astype(jnp.float32)
    mean_square = lax.optimization_barrier(jnp.mean(hidden * hidden, axis=1, keepdims=True))
    normed = (hidden * lax.rsqrt(mean_square + NORM_EPS) * norm_gain).astype(jnp.bfloat16)
    affinity = jax.nn.sigmoid(jnp.dot(normed, router_weight, preferred_element_type=jnp.float32))
    chosen = jnp.take_along_axis(affinity, expert_ids, axis=1)
    route = ROUTE_SCALE * chosen / lax.optimization_barrier(jnp.sum(chosen, axis=1, keepdims=True))
    onehot = expert_ids[:, :, None] == jnp.arange(EXPERTS, dtype=jnp.int32)[None, None, :]
    mixing = lax.optimization_barrier(jnp.sum(jnp.where(onehot, route[:, :, None], 0.0), axis=1))

    def one_expert(running, inputs):
        gate_matrix, up_matrix, down_matrix, mix_column = inputs
        gate = jnp.dot(normed, gate_matrix, preferred_element_type=jnp.float32)
        upward = jnp.dot(normed, up_matrix, preferred_element_type=jnp.float32)
        act = (jax.nn.silu(gate) * upward).astype(jnp.bfloat16)
        act_blocks = jnp.transpose(act.reshape(NEWTOK, FF // FFS, FFS), (1, 0, 2))
        down_blocks = down_matrix.reshape(FF // FFS, FFS, D)

        def add_block(accum, pair):
            block_out = jnp.dot(pair[0], pair[1], preferred_element_type=jnp.float32).astype(jnp.bfloat16)
            block_out = lax.optimization_barrier(block_out)
            return (accum + block_out.astype(jnp.float32), None)
        summed, ignored = lax.scan(add_block, jnp.zeros((NEWTOK, D), jnp.float32), (act_blocks, down_blocks))
        expert_out = lax.optimization_barrier(summed.astype(jnp.bfloat16)).astype(jnp.float32)
        return (running + mix_column[:, None] * expert_out, None)
    mixture, ignored = lax.scan(one_expert, jnp.zeros((NEWTOK, D), jnp.float32), (w_gate, w_up, w_down, mixing.T))
    return (hidden + mixture).astype(jnp.bfloat16)
```

```python
import functools
import math
import types

import jax
import jax.numpy as jnp
from jax import lax
from jax.experimental import pallas as pl
from jax.experimental.pallas import tpu as pltpu
from jax.sharding import PartitionSpec as P

QKD = 192
VMEM_BYTES = 56 * 1024 * 1024
SPARE_BYTES = 2 * 1024 * 1024

ROUTE_SCALE = 2.5
NORM_EPS = 1e-06


def block_position(row_index, block_order, block_rows):
    blocks = row_index // block_rows
    lookup = blocks[:, None] == jnp.arange(block_order.shape[0], dtype=jnp.int32)[None, :]
    leading = jnp.sum(jnp.where(lookup, block_order[None, :], 0), axis=1)
    return leading * block_rows + row_index % block_rows


def attend(query_lat, query_pe, keys, visible):
    row_count, head_count, latent_width = query_lat.shape
    key_count = keys.shape[1]
    pe_width = query_pe.shape[1] // head_count
    first_dot = jnp.dot(
        query_lat.reshape(row_count * head_count, latent_width),
        keys[:latent_width],
        preferred_element_type=jnp.float32,
    )
    second_dot = jnp.dot(
        query_pe.reshape(row_count * head_count, pe_width),
        keys[latent_width:],
        preferred_element_type=jnp.float32,
    )
    scores = ((first_dot + second_dot) * (1.0 / math.sqrt(QKD))).reshape(
        row_count, head_count, key_count
    )
    scores = jnp.where(visible[:, None, :], scores, -jnp.inf)
    row_max = jnp.max(scores, axis=2)
    exponent = jnp.exp(scores - row_max[:, :, None])
    row_sum = jnp.sum(exponent, axis=2)
    weights = exponent.astype(jnp.bfloat16).reshape(row_count * head_count, key_count)
    latent = lax.dot_general(
        weights, keys[:latent_width], (((1,), (1,)), ((), ())), preferred_element_type=jnp.float32
    )
    return (row_max, row_sum, latent.reshape(row_count, head_count, latent_width))


def remote(src, dst, send, recv, target):
    return pltpu.make_async_remote_copy(
        src_ref=src,
        dst_ref=dst,
        send_sem=send,
        recv_sem=recv,
        device_id=target,
        device_id_type=pl.DeviceIdType.MESH,
    )


def place():
    ctx_count, exp_count = lax.axis_size("ctx"), lax.axis_size("exp")
    ctx, exp = lax.axis_index("ctx"), lax.axis_index("exp")
    return ctx_count // 2, exp_count, ctx, exp, ctx // 2, ctx % 2


def greet(over_exp):
    ctx_count, exp_count = lax.axis_size("ctx"), lax.axis_size("exp")
    ctx, exp = lax.axis_index("ctx"), lax.axis_index("exp")
    barrier = pltpu.get_barrier_semaphore()
    peers = [((ctx + k) % ctx_count, exp) for k in range(1, ctx_count)]
    if over_exp:
        peers += [(ctx, (exp + k) % exp_count) for k in range(1, exp_count)]
    for peer in peers:
        pl.semaphore_signal(
            barrier, inc=1, device_id=peer, device_id_type=pl.DeviceIdType.MESH
        )
    pl.semaphore_wait(barrier, len(peers))


def column_block(rows, wide, ctx, exp, width):
    if not wide:
        return rows.at[ctx, exp]
    return rows.at[exp, :, pl.ds(pl.multiple_of(ctx * width, 128), width)]


def start_gather(src, out, send, recv):
    chips, _, ctx, exp, chip, core = place()
    flights = []
    for k in range(chips):
        peer = ctx + 1 - 2 * core if k == 0 else (chip + k) % chips * 2 + core
        copy = remote(src, out.at[ctx], send.at[0, k], recv.at[0, k], (peer, exp))
        copy.start()
        flights.append(copy)
    return flights


def finish_gather(out, flights, send, recv):
    chips, _, ctx, exp, chip, core = place()
    relayed = []
    for k in range(1, chips):
        flights[k].wait_recv()
        origin = (chip + chips - k) % chips * 2 + core
        copy = remote(
            out.at[origin], out.at[origin], send.at[1, k], recv.at[1, k], (ctx + 1 - 2 * core, exp)
        )
        copy.start()
        relayed.append(copy)
    flights[0].wait_recv()
    for copy in relayed:
        copy.wait_recv()
    for copy in flights + relayed:
        copy.wait_send()


def inputs_kernel(
    cache, fresh, res, ids, cache_out, fresh_out, res_out, ids_out,
    c_send, c_recv, f_send, f_recv, r_send, r_recv, i_send, i_recv, j_send, j_recv,
):
    chips, exp_count, ctx, exp, chip, core = place()
    ctx_count = 2 * chips
    greet(True)
    id_flights = []
    for k in range(1, exp_count):
        copy = remote(
            ids, ids_out.at[ctx, exp], i_send.at[k], i_recv.at[k], (ctx, (exp + k) % exp_count)
        )
        copy.start()
        id_flights.append(copy)
    cache_flights = start_gather(cache, cache_out, c_send, c_recv)
    fresh_flights = start_gather(fresh, fresh_out, f_send, f_recv)
    res_flights = []
    for k in range(1, ctx_count):
        peer = (ctx + k) % ctx_count
        copy = remote(res.at[peer], res_out.at[ctx], r_send.at[k], r_recv.at[k], (peer, exp))
        copy.start()
        res_flights.append(copy)
    cache_out[ctx] = cache[...]
    fresh_out[ctx] = fresh[...]
    res_out[ctx] = res[ctx]
    ids_out[ctx, exp] = ids[...]
    for copy in id_flights:
        copy.wait()
    for k in range(1, ctx_count):
        copy = remote(
            ids_out.at[ctx],
            ids_out.at[ctx],
            j_send.at[k],
            j_recv.at[k],
            ((ctx + k) % ctx_count, exp),
        )
        copy.start()
        res_flights.append(copy)
    finish_gather(cache_out, cache_flights, c_send, c_recv)
    finish_gather(fresh_out, fresh_flights, f_send, f_recv)
    for copy in res_flights:
        copy.wait()


def heads_kernel(src, out, send, recv):
    _, _, ctx, _, _, _ = place()
    greet(False)
    flights = start_gather(src, out, send, recv)
    out[ctx] = src[...]
    finish_gather(out, flights, send, recv)


def hidden_kernel(
    wide, part, res, out, landed, a_send, a_recv, b_send, b_recv, x_send, x_recv, f_send, f_recv
):
    chips, exp_count, ctx, exp, chip, core = place()
    partner = ctx + 1 - 2 * core
    width = part.shape[2]
    place_of = lambda c, e: column_block(out, wide, c, e, width)
    greet(True)
    first = []
    for k in range(1, exp_count):
        peer = (exp + k) % exp_count
        copy = remote(part.at[peer], landed.at[k], a_send.at[k], a_recv.at[k], (ctx, peer))
        copy.start()
        first.append(copy)
    total = part[exp].astype(jnp.float32)
    for k in range(1, exp_count):
        first[k - 1].wait_recv()
        total = total + landed[k].astype(jnp.float32)
    own = place_of(ctx, exp)
    own[...] = (res[...].astype(jnp.float32) + total).astype(jnp.bfloat16)
    pending = []
    spread = [None]
    for k in range(1, exp_count):
        copy = remote(
            own,
            own,
            b_send.at[k],
            b_recv.at[k],
            (ctx, (exp + k) % exp_count),
        )
        copy.start()
        spread.append(copy)
    for k in range(exp_count):
        if k > 0:
            spread[k].wait_recv()
        source = (exp + exp_count - k) % exp_count
        block = place_of(ctx, source)
        row = []
        for p in range(chips):
            peer = partner if p == 0 else (chip + p) % chips * 2 + core
            copy = remote(block, block, x_send.at[p, k], x_recv.at[p, k], (peer, exp))
            copy.start()
            row.append(copy)
        pending.append(row)
    last = []
    for k in range(exp_count):
        source = (exp + exp_count - k) % exp_count
        for p in range(1, chips):
            pending[k][p].wait_recv()
            origin = (chip + chips - p) % chips * 2 + core
            block = place_of(origin, source)
            copy = remote(block, block, f_send.at[p, k], f_recv.at[p, k], (partner, exp))
            copy.start()
            last.append(copy)
    for row in pending:
        row[0].wait_recv()
    for copy in last:
        copy.wait()
    for copy in first + spread[1:] + [copy for row in pending for copy in row]:
        copy.wait_send()


def combine_kernel(
    wide, y, hid, out, pair, cross_out, cross_in, home_out, home_in, final,
    p_send, p_recv, x_send, x_recv, e_send, e_recv, o_send, o_recv,
):
    chips, exp_count, ctx, exp, chip, core = place()
    partner = ctx + 1 - 2 * core
    ctx_count, tok, width = out.shape
    part_of = lambda c, e: column_block(y, wide, c, e, width)
    greet(True)
    order = list(range(1, exp_count)) + [0]
    halves, crossing, homing = {}, {}, {}
    for k in order:
        dest = (exp + k) % exp_count
        for j in list(range(1, chips)) + [0]:
            theirs = (chip + j) % chips * 2 + 1 - core
            copy = remote(
                part_of(theirs, dest),
                pair.at[k, j],
                p_send.at[k, j],
                p_recv.at[k, j],
                (partner, exp),
            )
            copy.start()
            halves[k, j] = copy
    for k in order:
        dest = (exp + k) % exp_count
        for j in range(1, chips):
            owner = (chip + j) % chips * 2 + core
            halves[k, j].wait_recv()
            both = part_of(owner, dest)[...].astype(jnp.float32) + pair[k, j].astype(jnp.float32)
            cross_out[k, j] = both.astype(jnp.bfloat16)
            copy = remote(
                cross_out.at[k, j],
                cross_in.at[k, j],
                x_send.at[k, j],
                x_recv.at[k, j],
                (owner, exp),
            )
            copy.start()
            crossing[k, j] = copy
    total = hid[...].astype(jnp.float32)
    for k in order:
        dest = (exp + k) % exp_count
        halves[k, 0].wait_recv()
        both = part_of(ctx, dest)[...].astype(jnp.float32) + pair[k, 0].astype(jnp.float32)
        for j in range(1, chips):
            crossing[k, j].wait_recv()
            both = both + cross_in[k, j].astype(jnp.float32)
        if k == 0:
            total = total + both
        else:
            home_out[k] = both.astype(jnp.bfloat16)
            copy = remote(
                home_out.at[k], home_in.at[k], e_send.at[k], e_recv.at[k], (ctx, dest)
            )
            copy.start()
            homing[k] = copy
    for k in range(1, exp_count):
        homing[k].wait_recv()
        total = total + home_in[k].astype(jnp.float32)
    for c in range(ctx_count):
        final[c] = total[c * tok : (c + 1) * tok].astype(jnp.bfloat16)
    last = []
    for k in range(1, ctx_count):
        peer = (ctx + k) % ctx_count
        copy = remote(final.at[peer], out.at[ctx], o_send.at[k], o_recv.at[k], (peer, exp))
        copy.start()
        last.append(copy)
    out[ctx] = final[ctx]
    for copy in last:
        copy.wait()
    for copy in list(halves.values()) + list(crossing.values()) + list(homing.values()):
        copy.wait_send()


def exchange(number, kernel, shapes, scratch, *operands):
    vmem = pl.BlockSpec(memory_space=pltpu.VMEM)
    held = jax.tree.leaves(shapes) + list(operands)
    held += [s for s in scratch if s.dtype == jnp.bfloat16]
    need = sum(2 * math.prod(h.shape) * h.dtype.itemsize for h in held) + SPARE_BYTES
    return pl.pallas_call(
        kernel,
        out_shape=shapes,
        in_specs=[vmem] * len(operands),
        out_specs=jax.tree.map(lambda _: vmem, shapes),
        scratch_shapes=scratch,
        compiler_params=pltpu.CompilerParams(
            collective_id=number, has_side_effects=True, vmem_limit_bytes=min(need, VMEM_BYTES)
        ),
    )(*operands)


def staged_body(
    q_nope,
    q_rope,
    cache_keys,
    fresh_keys,
    block_order,
    w_uv,
    w_out,
    residual,
    norm_gain,
    router_weight,
    expert_ids,
    w_gate,
    w_up,
    w_down,
):
    ctx_count = lax.axis_size("ctx")
    exp_count = lax.axis_size("exp")
    ctx_index = lax.axis_index("ctx")
    exp_index = lax.axis_index("exp")
    rows_here, heads_here, latent_width = q_nope.shape
    value_width = w_uv.shape[2]
    key_width, cache_len = cache_keys.shape
    tok_here, model_width = residual.shape
    col_part = w_out.shape[1]
    chips = ctx_count // 2
    block_rows = rows_here * ctx_count // block_order.shape[0]
    dma = pltpu.SemaphoreType.DMA
    bf16 = functools.partial(jax.ShapeDtypeStruct, dtype=jnp.bfloat16)

    res_cols = residual.reshape(tok_here, ctx_count, col_part).transpose(1, 0, 2)
    cache_all, fresh_all, res_own, ids_all = exchange(
        0,
        inputs_kernel,
        (
            bf16((ctx_count, key_width, cache_len)),
            bf16((ctx_count, rows_here, key_width)),
            bf16((ctx_count, tok_here, col_part)),
            jax.ShapeDtypeStruct((ctx_count, exp_count) + expert_ids.shape, jnp.int32),
        ),
        [dma((2, chips))] * 4 + [dma((ctx_count,))] * 2 + [dma((exp_count,))] * 2
        + [dma((ctx_count,))] * 2,
        cache_keys, fresh_keys.T, res_cols, expert_ids,
    )
    cached = jnp.transpose(cache_all, (1, 0, 2)).reshape(key_width, ctx_count * cache_len)
    fresh = fresh_all.reshape(ctx_count * rows_here, key_width).T
    keys = jnp.concatenate([cached, fresh], axis=1)
    own_rows = ctx_index * rows_here + jnp.arange(rows_here, dtype=jnp.int32)
    own_pos = block_position(own_rows, block_order, block_rows)
    new_rows = jnp.arange(ctx_count * rows_here, dtype=jnp.int32)
    key_pos = jnp.concatenate(
        [
            jnp.full((ctx_count * cache_len,), -1, jnp.int32),
            block_position(new_rows, block_order, block_rows),
        ]
    )
    visible = key_pos[None, :] <= own_pos[:, None]
    row_max, row_sum, latent = attend(q_nope, q_rope, keys, visible)
    normal_lat = (latent / row_sum[:, :, None]).astype(jnp.bfloat16)
    head_out = jnp.einsum(
        "rhl,hlv->rhv", normal_lat, w_uv, preferred_element_type=jnp.float32
    ).astype(jnp.bfloat16).reshape(rows_here, heads_here * value_width)
    heads_all = exchange(
        1,
        heads_kernel,
        bf16((ctx_count,) + head_out.shape),
        [dma((2, chips))] * 2,
        head_out,
    )
    heads_all = (
        heads_all.reshape(ctx_count, exp_count, tok_here, -1)
        .transpose(1, 0, 2, 3)
        .reshape(exp_count * ctx_count * tok_here, -1)
    )
    head_partial = jnp.dot(heads_all, w_out, preferred_element_type=jnp.float32)
    group = ctx_count * tok_here
    wide = col_part % 128 == 0
    tokens = exp_count * group
    stripes = (exp_count, group, model_width)
    blocks = (ctx_count, exp_count, group, col_part)
    hidden_all = exchange(
        2,
        functools.partial(hidden_kernel, wide),
        bf16(stripes if wide else blocks),
        [pltpu.VMEM((exp_count, group, col_part), jnp.bfloat16)]
        + [dma((exp_count,))] * 4
        + [dma((chips, exp_count))] * 4,
        head_partial.astype(jnp.bfloat16).reshape(exp_count, group, col_part),
        res_own.reshape(group, col_part),
    )
    if not wide:
        hidden_all = hidden_all.transpose(1, 2, 0, 3)
    hidden_rows = hidden_all.reshape(tokens, model_width)
    hidden = hidden_rows.astype(jnp.float32)
    mean_square = jnp.mean(hidden * hidden, axis=1, keepdims=True)
    normed = (hidden * lax.rsqrt(mean_square + NORM_EPS) * norm_gain).astype(jnp.bfloat16)
    affinity = jax.nn.sigmoid(jnp.dot(normed, router_weight, preferred_element_type=jnp.float32))
    expert_count = router_weight.shape[1]
    ids = ids_all.transpose(1, 0, 2, 3).reshape(tokens, -1)
    onehot = ids[:, :, None] == jnp.arange(expert_count, dtype=jnp.int32)[None, None, :]
    named = jnp.any(onehot, axis=1)
    chosen = jnp.where(named, affinity, 0.0)
    mixing = ROUTE_SCALE * chosen / jnp.sum(chosen, axis=1, keepdims=True)
    local_experts, _, hidden_units = w_gate.shape
    mine = lax.dynamic_slice_in_dim(mixing, exp_index * local_experts, local_experts, axis=1)
    acts = []
    for i in range(local_experts):
        gate = jnp.dot(normed, w_gate[i], preferred_element_type=jnp.float32)
        upward = jnp.dot(normed, w_up[i], preferred_element_type=jnp.float32)
        acts.append((jax.nn.silu(gate) * upward * mine[:, i : i + 1]).astype(jnp.bfloat16))
    acts = jnp.concatenate(acts, axis=1)
    down = w_down.reshape(local_experts * hidden_units, model_width)
    mixed = jnp.dot(acts, down, preferred_element_type=jnp.float32).astype(jnp.bfloat16)
    own_hidden = lax.dynamic_slice(
        hidden_rows, (exp_index * group, ctx_index * col_part), (group, col_part)
    )
    mixed = mixed.reshape(stripes)
    if not wide:
        mixed = mixed.reshape(exp_count, group, ctx_count, col_part).transpose(2, 0, 1, 3)
    block = (group, col_part)
    owned = exchange(
        3,
        functools.partial(combine_kernel, wide),
        bf16((ctx_count, tok_here, col_part)),
        [pltpu.VMEM((exp_count, chips) + block, jnp.bfloat16)] * 3
        + [pltpu.VMEM((exp_count,) + block, jnp.bfloat16)] * 2
        + [pltpu.VMEM((ctx_count, tok_here, col_part), jnp.bfloat16)]
        + [dma((exp_count, chips))] * 4
        + [dma((exp_count,))] * 2
        + [dma((ctx_count,))] * 2,
        mixed,
        own_hidden,
    )
    return owned.transpose(1, 0, 2).reshape(tok_here, model_width)


GROUPS = 4
FOLD = 2


def widths(total, unit, parts):
    tiles = total // unit
    return [(tiles // parts + (1 if i < tiles % parts else 0)) * unit for i in range(parts)]


def offsets(sizes):
    return [sum(sizes[:i]) for i in range(len(sizes))]


def fits(ctx_count, exp_count, q_nope, cache_keys, w_uv, w_out, residual, w_gate, block_rows):
    rows, heads, lat = q_nope.shape
    weights = 2 * (math.prod(w_uv.shape) + math.prod(w_out.shape) + 3 * math.prod(w_gate.shape))
    return (
        ctx_count == 4
        and exp_count % FOLD == 0
        and residual.shape[0] * exp_count == rows
        and residual.shape[0] * ctx_count % 8 == 0
        and heads % GROUPS == 0
        and rows % 16 == 0
        and rows % block_rows == 0
        and w_out.shape[1] % 256 == 0
        and cache_keys.shape[1] % 128 == 0
        and lat % 128 == 0
        and w_gate.shape[2] % 128 == 0
        and weights < 54 * 1024 * 1024
        and residual.shape[1] % 1024 == 0
        and w_out.shape[1] >= 1024
        and residual.shape[1] // 1024 * rows * ctx_count <= w_out.shape[0]
    )


def onehot(shape, source):
    row = lax.broadcasted_iota(jnp.int32, shape, 0)
    col = lax.broadcasted_iota(jnp.int32, shape, 1)
    return jnp.where(col == source(row), 1.0, 0.0).astype(jnp.bfloat16)


def mm(a, b):
    return jnp.dot(a, b, preferred_element_type=jnp.float32)


def mm_t(a, b):
    return lax.dot_general(a, b, (((1,), (1,)), ((), ())), preferred_element_type=jnp.float32)


def fused_kernel(
    names, dims,
    q_nope, q_rope, cache, fresh, order, w_uv, w_out, res, gain, router, ids, w_gate, w_up, w_down,
    out, *refs,
):
    s = types.SimpleNamespace(**dict(zip(names, refs)))
    d = dims
    bf16, f32 = jnp.bfloat16, jnp.float32
    ctx, exp = lax.axis_index("ctx"), lax.axis_index("exp")
    C, E, Z = d.ctx_count, d.exp_count, d.exp_count // FOLD
    x, core = ctx // 2, ctx % 2
    z, y = exp // FOLD, exp % FOLD
    xctx = (1 - x) * 2 + core
    partner = (ctx + 1 - 2 * core, exp)
    xpeer = (xctx, exp)
    ypeer = (ctx, z * FOLD + 1 - y)
    zpeer = lambda j: (ctx, (z + j) % Z * FOLD + y)
    rows, heads, lat, rope = d.rows, d.heads, d.lat, d.rope
    vals, col, tok, tokens = d.vals, d.col, d.tok, d.tokens
    group = C * tok
    hg = heads // GROUPS
    sent = []

    def push(src, dst, sems, index, target):
        send, recv = sems
        copy = remote(src, dst, send.at[index], recv.at[index], target)
        copy.start()
        sent.append(copy)
        return copy

    def load(src, dst, index):
        copy = pltpu.make_async_copy(src, dst, s.load.at[index])
        copy.start()
        return copy

    lanes = lambda start, size: pl.ds(pl.multiple_of(start, 128), size)

    l_cache = load(cache, s.kall.at[:, lanes(ctx * d.cached, d.cached)], 0)
    l_fresh = load(fresh, s.kfresh.at[pl.ds(pl.multiple_of(ctx * rows, 16), rows)], 1)
    l_res = load(res, s.res, 2)
    l_ids = load(ids, s.ids, 3)
    l_order = load(order, s.order, 4)
    l_q = load(q_nope, s.qn, 5)
    l_qr = load(q_rope, s.qr, 6)
    l_uv = load(w_uv, s.wuv, 7)
    l_gain = load(gain, s.gain, 8)
    l_router = load(router, s.router, 9)
    l_out = load(w_out, s.wout, 10)
    l_gate = load(w_gate, s.wg, 11)
    l_up = load(w_up, s.wu, 12)
    l_down = load(w_down, s.wd, 13)
    greet(True)

    l_cache.wait()
    l_fresh.wait()
    key_sems = (s.k_send, s.k_recv)

    def send_keys(owner, index, target):
        a = s.kall.at[:, lanes(owner * d.cached, d.cached)]
        b = s.kfresh.at[pl.ds(pl.multiple_of(owner * rows, 16), rows)]
        return [push(a, a, key_sems, (0, index), target), push(b, b, key_sems, (1, index), target)]

    k_cross = send_keys(ctx, 0, xpeer)
    k_pair = send_keys(ctx, 1, partner)

    l_res.wait()
    r_flights = []
    for k in range(1, C):
        peer = (ctx + k) % C
        r_flights.append(
            push(s.res.at[:, lanes(peer * col, col)], s.rin.at[ctx], (s.r_send, s.r_recv), k, (peer, exp))
        )
    s.rin[ctx] = s.res[:, lanes(ctx * col, col)]
    l_ids.wait()
    named = jnp.zeros((tok, 128), f32)
    lane = lax.broadcasted_iota(jnp.int32, (tok, 128), 1)
    for k in range(d.top):
        named = named + jnp.where(s.ids[:, k : k + 1] == lane, 1.0, 0.0)
    s.nsrc[...] = jnp.zeros((8, 128), f32)
    s.nsrc[0:tok, :] = named
    n_flights = [
        push(s.nsrc, s.nall.at[exp, ctx], (s.n_send, s.n_recv), k, (ctx, (exp + k) % E))
        for k in range(1, E)
    ]
    s.nall[exp, ctx] = s.nsrc[...]

    l_q.wait()
    for g in range(GROUPS):
        part = hg * rows
        perm = onehot((part, rows * heads), lambda i: (i % rows) * heads + g * hg + i // rows)
        s.qh[g * part : (g + 1) * part, :] = mm(perm, s.qn[...]).astype(bf16)
    l_qr.wait()
    for h in range(heads):
        s.qrh[h * rows : (h + 1) * rows, :] = s.qr[:, h * rope : (h + 1) * rope]

    l_order.wait()
    size = d.block
    own_blocks = rows // size
    part = hg * rows
    row_id = lax.broadcasted_iota(jnp.int32, (part, tokens), 0) % rows
    key_id = lax.broadcasted_iota(jnp.int32, (part, tokens), 1)
    own_pos = row_id % size
    key_pos = key_id % size
    for b in range(own_blocks):
        own_pos = own_pos + jnp.where(row_id // size == b, s.order[ctx * own_blocks + b] * size, 0)
    for b in range(tokens // size):
        key_pos = key_pos + jnp.where(key_id // size == b, s.order[b] * size, 0)
    s.bias[...] = jnp.where(key_pos <= own_pos, 0.0, -jnp.inf)

    for copy in n_flights:
        copy.wait_recv()
    n_last = []
    for k in range(1, C):
        view = s.nall.at[:, ctx]
        n_last.append(push(view, view, (s.m_send, s.m_recv), k, ((ctx + k) % C, exp)))

    for copy in k_cross:
        copy.wait_recv()
    k_far = send_keys(xctx, 2, partner)
    for copy in k_pair + k_far:
        copy.wait_recv()

    scale = 1.0 / math.sqrt(QKD)
    l_uv.wait()
    h_cross, h_pair = [], []
    for g in range(GROUPS):
        q = s.qh[g * part : (g + 1) * part, :]
        qr = s.qrh[g * part : (g + 1) * part, :]
        old = (mm(q, s.kall[0:lat, :]) + mm(qr, s.kall[lat : lat + rope, :])) * scale
        new = (mm_t(q, s.kfresh[:, 0:lat]) + mm_t(qr, s.kfresh[:, lat : lat + rope])) * scale
        new = new + s.bias[...]
        top = jnp.maximum(jnp.max(old, axis=1, keepdims=True), jnp.max(new, axis=1, keepdims=True))
        old = jnp.exp(old - top)
        new = jnp.exp(new - top)
        total = jnp.sum(old, axis=1, keepdims=True) + jnp.sum(new, axis=1, keepdims=True)
        latent = mm_t(old.astype(bf16), s.kall[0:lat, :]) + mm(new.astype(bf16), s.kfresh[:, 0:lat])
        latent = (latent / total).astype(bf16)
        for h in range(hg):
            one = mm(latent[h * rows : (h + 1) * rows], s.wuv[g * hg + h])
            s.heads[ctx, g, :, h * vals : (h + 1) * vals] = one.astype(bf16)
        view = s.heads.at[ctx, g]
        h_cross.append(push(view, view, (s.h_send, s.h_recv), (0, g), xpeer))
        h_pair.append(push(view, view, (s.h_send, s.h_recv), (1, g), partner))
    h_far = []
    for g in range(GROUPS):
        h_cross[g].wait_recv()
        view = s.heads.at[xctx, g]
        h_far.append(push(view, view, (s.h_send, s.h_recv), (2, g), partner))

    l_out.wait()
    deep = hg * vals
    for g in range(GROUPS):
        h_pair[g].wait_recv()
        h_far[g].wait_recv()
        value = mm(s.heads[:, g].reshape(tokens, deep), s.wout[g * deep : (g + 1) * deep, :])
        if g == 0:
            s.pacc[...] = value
        else:
            s.pacc[...] = s.pacc[...] + value

    chunks = d.chunks
    starts = offsets(chunks)
    to_group = onehot(
        (tokens, tokens), lambda i: (i // tok) % C * rows + i // group * tok + i % tok
    )
    y_flights = []
    for q, (o, w) in enumerate(zip(starts, chunks)):
        value = mm(to_group, s.pacc[:, o : o + w].astype(bf16)).astype(bf16)
        s.p[:, :, :, o : o + w] = value.reshape(Z, FOLD, group, w)
        y_flights.append(
            push(
                s.p.at[:, 1 - y, :, pl.ds(o, w)], s.yin.at[:, :, pl.ds(o, w)],
                (s.y_send, s.y_recv), q, ypeer,
            )
        )
    z_flights = []
    for q, (o, w) in enumerate(zip(starts, chunks)):
        y_flights[q].wait_recv()
        both = s.p[:, y, :, o : o + w].astype(f32) + s.yin[:, :, o : o + w].astype(f32)
        s.zsrc[:, :, o : o + w] = both.astype(bf16)
        z_flights.append([
            push(
                s.zsrc.at[(z + j) % Z, :, pl.ds(o, w)], s.zin.at[j, :, pl.ds(o, w)],
                (s.z_send, s.z_recv), (q, j), zpeer(j),
            )
            for j in range(1, Z)
        ])
    for copy in r_flights:
        copy.wait_recv()
    for c in range(C):
        s.rsum[c * tok : (c + 1) * tok, :] = s.rin[c].astype(f32)

    def block(c, e, q):
        return s.hid.at[e, :, lanes(c * col + starts[q], chunks[q])]

    gather = {}

    def spread(q, step, index, c, e, target):
        view = block(c, e, q)
        gather[q, step, index] = push(view, view, (s.g_send, s.g_recv), (q, d.slot[step, index]), target)

    def axes(q):
        return (ypeer, xpeer) if q % 2 == 0 else (xpeer, ypeer)

    def near(q, j):
        return ctx, (z + Z - j) % Z * FOLD + y

    def first(q, j):
        c, e = near(q, j)
        return (c, e + 1 - 2 * y) if q % 2 == 0 else (xctx, e)

    def second(q, i):
        if q % 2 == 0:
            return xctx, (near(q, i) if i < Z else first(q, i - Z))[1]
        c, e = near(q, i) if i < Z else first(q, i - Z)
        return c, e + 1 - 2 * y

    def open_gather(q):
        c, e = near(q, 0)
        for j in range(1, Z):
            spread(q, "z", j, c, e, zpeer(j))
        a, b = axes(q)
        spread(q, "a", 0, c, e, a)
        spread(q, "b", 0, c, e, b)
        spread(q, "d", 0, c, e, partner)

    def pass_near(q):
        a, b = axes(q)
        for j in range(1, Z):
            gather[q, "z", j].wait_recv()
            c, e = near(q, j)
            spread(q, "a", j, c, e, a)
            spread(q, "b", j, c, e, b)
            spread(q, "d", j, c, e, partner)

    def pass_first(q):
        _, b = axes(q)
        for j in range(Z):
            gather[q, "a", j].wait_recv()
            c, e = first(q, j)
            spread(q, "b", Z + j, c, e, b)
            spread(q, "d", Z + j, c, e, partner)

    def pass_second(q):
        for i in range(2 * Z):
            gather[q, "b", i].wait_recv()
            c, e = second(q, i)
            spread(q, "d", 2 * Z + i, c, e, partner)

    def close_gather(q):
        for i in range(4 * Z):
            gather[q, "d", i].wait_recv()

    for q, (o, w) in enumerate(zip(starts, chunks)):
        for copy in z_flights[q]:
            copy.wait_recv()
        both = s.p[z, y, :, o : o + w].astype(f32) + s.yin[z, :, o : o + w].astype(f32)
        for j in range(1, Z):
            both = both + s.zin[j, :, o : o + w].astype(f32)
        both = both + s.rsum[:, o : o + w]
        s.hid[exp, :, lanes(ctx * col + o, w)] = both.astype(bf16)
        open_gather(q)

    l_gain.wait()
    l_router.wait()
    l_gate.wait()
    l_up.wait()
    s.ss[...] = jnp.zeros(s.ss.shape, f32)
    s.racc[...] = jnp.zeros(s.racc.shape, f32)
    s.gacc[...] = jnp.zeros(s.gacc.shape, f32)
    s.uacc[...] = jnp.zeros(s.uacc.shape, f32)
    units = d.units

    def consume(q):
        w = chunks[q]

        def one(i, carry):
            c = (ctx + i) % C
            at = lanes(c * col + starts[q], w)
            hidden = s.hid[:, :, at].reshape(tokens, w).astype(f32)
            square = hidden * hidden
            some = square[:, 0:128]
            for k in range(1, w // 128):
                some = some + square[:, k * 128 : (k + 1) * 128]
            s.ss[...] = s.ss[...] + some
            scaled = (hidden * s.gain[:, at]).astype(bf16)
            s.racc[...] = s.racc[...] + mm_t(scaled, s.router[:, at])
            for k in range(d.local):
                here = slice(k * units, (k + 1) * units)
                s.gacc[:, here] = s.gacc[:, here] + mm(scaled, s.wg[k, at, :])
                s.uacc[:, here] = s.uacc[:, here] + mm(scaled, s.wu[k, at, :])
            return carry

        lax.fori_loop(0, C, one, 0)

    count = len(chunks)
    for q in range(count):
        pass_near(q)
        pass_first(q)
    for q in range(count):
        pass_second(q)
        close_gather(q)
        if q > 0:
            consume(q - 1)
    consume(count - 1)

    for copy in n_last:
        copy.wait_recv()
    squeeze = onehot((tokens, tokens // tok * 8), lambda i: i // tok * 8 + i % tok)
    named = mm(squeeze, s.nall[...].reshape(tokens // tok * 8, 128).astype(bf16))
    named = named[:, 0 : d.experts]
    mean = jnp.sum(s.ss[...], axis=1, keepdims=True) * (1.0 / d.width)
    factor = lax.rsqrt(mean + NORM_EPS)
    affinity = jax.nn.sigmoid(s.racc[...] * factor)
    chosen = jnp.where(named > 0.5, affinity, 0.0)
    mixing = ROUTE_SCALE * chosen / jnp.sum(chosen, axis=1, keepdims=True)
    which = lax.broadcasted_iota(jnp.int32, (tokens, d.experts), 1)
    for k in range(d.local):
        here = slice(k * units, (k + 1) * units)
        mine = jnp.sum(jnp.where(which == exp * d.local + k, mixing, 0.0), axis=1, keepdims=True)
        gate = s.gacc[:, here] * factor
        upward = s.uacc[:, here] * factor
        s.acts[:, here] = (gate * jax.nn.sigmoid(gate) * upward * mine).astype(bf16)

    def owner_order(i):
        t, zz, yy = i % tok, i // tok % Z, i // (tok * Z) % FOLD
        xx, kk = i // (tok * Z * FOLD) % 2, i // (tok * Z * FOLD * 2)
        return (zz * FOLD + yy) * group + (xx * 2 + kk) * tok + t

    to_owner = onehot((tokens, tokens), owner_order)
    for k in range(d.local):
        here = slice(k * units, (k + 1) * units)
        s.acts[:, here] = mm(to_owner, s.acts[:, here]).astype(bf16)
    l_down.wait()
    cw, n = d.out_width, d.width // d.out_width
    half, quarter, eighth = tokens // 2, tokens // 4, tokens // 8
    pairs, hops, lasts, ends = {}, {}, {}, {}

    def produce(i):
        mixed = mm(s.acts[...], s.wd[:, i * cw : (i + 1) * cw]).astype(bf16)
        s.wout[i * tokens : (i + 1) * tokens, 0:cw] = mixed
        away = s.wout.at[pl.ds(pl.multiple_of(i * tokens + (1 - core) * half, 16), half), pl.ds(0, cw)]
        pairs[i] = push(away, s.pair.at[i], (s.p_send, s.p_recv), i, partner)

    def join_pair(i):
        pairs[i].wait_recv()
        mine = s.wout[pl.ds(pl.multiple_of(i * tokens + core * half, 16), half), 0:cw]
        both = mine.astype(f32) + s.pair[i].astype(f32)
        s.s1[i] = both.astype(bf16).reshape(2, FOLD, eighth, cw)
        if i % 2 == 0:
            hops[i] = push(s.s1.at[i, 1 - x], s.h1.at[i], (s.a_send, s.a_recv), i, xpeer)
        else:
            hops[i] = push(s.s1.at[i, :, 1 - y], s.h1.at[i], (s.a_send, s.a_recv), i, ypeer)

    def join_hop(i):
        hops[i].wait_recv()
        mine = s.s1[i, x] if i % 2 == 0 else s.s1[i, :, y]
        s.s2[i] = (mine.astype(f32) + s.h1[i].astype(f32)).astype(bf16)
        if i % 2 == 0:
            lasts[i] = push(s.s2.at[i, 1 - y], s.h2.at[i], (s.b_send, s.b_recv), i, ypeer)
        else:
            lasts[i] = push(s.s2.at[i, 1 - x], s.h2.at[i], (s.b_send, s.b_recv), i, xpeer)

    def join_last(i):
        lasts[i].wait_recv()
        mine = s.s2[i, y] if i % 2 == 0 else s.s2[i, x]
        s.total[...] = mine.astype(f32) + s.h2[i].astype(f32)
        for zz in range(Z):
            s.zo[i, zz] = s.total[zz * tok : (zz + 1) * tok, :].astype(bf16)
        ends[i] = [
            push(s.zo.at[i, (z + j) % Z], s.zi.at[i, j], (s.e_send, s.e_recv), (i, j), zpeer(j))
            for j in range(1, Z)
        ]

    def finish(i):
        at = slice(i * cw, (i + 1) * cw)
        s.total[...] = s.hid[exp, :, at].astype(f32)
        value = s.zo[i, z].astype(f32)
        for c in range(C):
            value = value + jnp.where(ctx == c, s.total[c * tok : (c + 1) * tok, :], 0.0)
        for j in range(1, Z):
            ends[i][j - 1].wait_recv()
            value = value + s.zi[i, j].astype(f32)
        out[:, at] = value.astype(bf16)

    lag = 3
    for i in range(n):
        produce(i)
        if i >= lag:
            join_pair(i - lag)
    for i in range(max(n - lag, 0), n):
        join_pair(i)
    for i in range(n):
        join_hop(i)
    for i in range(n):
        join_last(i)
    for i in range(n):
        finish(i)
    for copy in sent:
        copy.wait_send()


def fused_body(dims, arguments):
    (
        q_nope, q_rope, cache_keys, fresh_keys, block_order, w_uv, w_out, residual, norm_gain,
        router_weight, expert_ids, w_gate, w_up, w_down,
    ) = arguments
    d = dims
    bf16, f32 = jnp.bfloat16, jnp.float32
    dma = pltpu.SemaphoreType.DMA
    vmem = pltpu.VMEM
    C, E, Z, Y = d.ctx_count, d.exp_count, d.exp_count // FOLD, FOLD
    group = C * d.tok
    keys = d.lat + d.rope
    n = d.width // d.out_width
    queries = d.rows * d.heads
    part = queries // GROUPS
    hidden = d.local * d.units
    q = len(d.chunks)
    scratch = dict(
        wuv=vmem(w_uv.shape, bf16),
        wout=vmem(w_out.shape, bf16),
        wg=vmem(w_gate.shape, bf16),
        wu=vmem(w_up.shape, bf16),
        wd=vmem((hidden, d.width), bf16),
        qn=vmem((queries, d.lat), bf16),
        qh=vmem((queries, d.lat), bf16),
        qr=vmem(q_rope.shape, bf16),
        qrh=vmem((queries, d.rope), bf16),
        kall=vmem((keys, C * d.cached), bf16),
        kfresh=vmem((d.tokens, keys), bf16),
        bias=vmem((part, d.tokens), f32),
        res=vmem(residual.shape, bf16),
        rin=vmem((C, d.tok, d.col), bf16),
        rsum=vmem((group, d.col), f32),
        ids=vmem(expert_ids.shape, jnp.int32),
        nsrc=vmem((8, 128), f32),
        nall=vmem((E, C, 8, 128), f32),
        order=pltpu.SMEM(block_order.shape, jnp.int32),
        gain=vmem((1, d.width), f32),
        router=vmem((d.experts, d.width), bf16),
        heads=vmem((C, GROUPS, d.rows, d.heads // GROUPS * d.vals), bf16),
        pacc=vmem((d.tokens, d.col), f32),
        p=vmem((Z, Y, group, d.col), bf16),
        yin=vmem((Z, group, d.col), bf16),
        zsrc=vmem((Z, group, d.col), bf16),
        zin=vmem((Z, group, d.col), bf16),
        hid=vmem((E, group, d.width), bf16),
        ss=vmem((d.tokens, 128), f32),
        racc=vmem((d.tokens, d.experts), f32),
        gacc=vmem((d.tokens, hidden), f32),
        uacc=vmem((d.tokens, hidden), f32),
        acts=vmem((d.tokens, hidden), bf16),
        pair=vmem((n, d.tokens // 2, d.out_width), bf16),
        s1=vmem((n, 2, Y, d.tokens // 8, d.out_width), bf16),
        h1=vmem((n, 2, d.tokens // 8, d.out_width), bf16),
        s2=vmem((n, 2, d.tokens // 8, d.out_width), bf16),
        h2=vmem((n, d.tokens // 8, d.out_width), bf16),
        total=vmem((d.tokens // 8, d.out_width), f32),
        zo=vmem((n, Z, d.tok, d.out_width), bf16),
        zi=vmem((n, Z, d.tok, d.out_width), bf16),
        load=dma((14,)),
        k_send=dma((2, 3)), k_recv=dma((2, 3)),
        r_send=dma((C,)), r_recv=dma((C,)),
        n_send=dma((E,)), n_recv=dma((E,)),
        m_send=dma((C,)), m_recv=dma((C,)),
        h_send=dma((3, GROUPS)), h_recv=dma((3, GROUPS)),
        y_send=dma((q,)), y_recv=dma((q,)),
        z_send=dma((q, Z)), z_recv=dma((q, Z)),
        g_send=dma((q, len(d.slot))), g_recv=dma((q, len(d.slot))),
        p_send=dma((n,)), p_recv=dma((n,)),
        a_send=dma((n,)), a_recv=dma((n,)),
        b_send=dma((n,)), b_recv=dma((n,)),
        e_send=dma((n, Z)), e_recv=dma((n, Z)),
    )
    anywhere = pl.BlockSpec(memory_space=pl.ANY)
    operands = (
        q_nope.reshape(queries, d.lat), q_rope, cache_keys, fresh_keys.T, block_order, w_uv, w_out,
        residual, norm_gain.reshape(1, -1), router_weight.T, expert_ids, w_gate, w_up,
        w_down.reshape(hidden, d.width),
    )
    return pl.pallas_call(
        functools.partial(fused_kernel, tuple(scratch), d),
        out_shape=jax.ShapeDtypeStruct(residual.shape, bf16),
        in_specs=[anywhere] * len(operands),
        out_specs=pl.BlockSpec(memory_space=pltpu.VMEM),
        scratch_shapes=list(scratch.values()),
        compiler_params=pltpu.CompilerParams(
            collective_id=0, has_side_effects=True, vmem_limit_bytes=67043328
        ),
    )(*operands)


def body(*arguments):
    (
        q_nope, q_rope, cache_keys, _, block_order, w_uv, w_out, residual, _, router_weight,
        expert_ids, w_gate, _, _,
    ) = arguments
    ctx_count, exp_count = lax.axis_size("ctx"), lax.axis_size("exp")
    rows, heads, lat = q_nope.shape
    tokens = rows * ctx_count
    block = tokens // block_order.shape[0]
    if not fits(ctx_count, exp_count, q_nope, cache_keys, w_uv, w_out, residual, w_gate, block):
        return staged_body(*arguments)
    depth = exp_count // FOLD
    steps = [("z", j) for j in range(1, depth)] + [("a", j) for j in range(depth)]
    steps += [("b", j) for j in range(2 * depth)] + [("d", j) for j in range(4 * depth)]
    width = residual.shape[1]
    dims = types.SimpleNamespace(
        ctx_count=ctx_count, exp_count=exp_count, rows=rows, heads=heads, lat=lat,
        rope=q_rope.shape[1] // heads, vals=w_uv.shape[2], col=w_out.shape[1],
        tok=residual.shape[0], tokens=tokens, cached=cache_keys.shape[1], top=expert_ids.shape[1],
        block=block, experts=router_weight.shape[1], local=w_gate.shape[0], units=w_gate.shape[2],
        width=width, chunks=widths(w_out.shape[1], 256, 2),
        out_width=1024,
        slot={step: i for i, step in enumerate(steps)},
    )
    return fused_body(dims, arguments)


def solution(mesh):
    return jax.shard_map(
        body,
        mesh=mesh,
        in_specs=(
            P("ctx", "exp", None),
            P("ctx", "exp"),
            P(None, "ctx"),
            P(None, "ctx"),
            P(),
            P("exp", None, None),
            P("exp", "ctx"),
            P(("ctx", "exp"), None),
            P(),
            P(),
            P(("ctx", "exp"), None),
            P("exp", None, "ctx"),
            P("exp", None, "ctx"),
            P("exp", "ctx", None),
        ),
        out_specs=P(("ctx", "exp"), None),
        check_vma=False,
    )
```

```python
import functools
import math
import types

import jax
import jax.numpy as jnp
from jax import lax
from jax.experimental import pallas as pl
from jax.experimental.pallas import tpu as pltpu
from jax.sharding import PartitionSpec as P

QKD = 192
VMEM_BYTES = 56 * 1024 * 1024
SPARE_BYTES = 2 * 1024 * 1024

ROUTE_SCALE = 2.5
NORM_EPS = 1e-06


def block_position(row_index, block_order, block_rows):
    blocks = row_index // block_rows
    lookup = blocks[:, None] == jnp.arange(block_order.shape[0], dtype=jnp.int32)[None, :]
    leading = jnp.sum(jnp.where(lookup, block_order[None, :], 0), axis=1)
    return leading * block_rows + row_index % block_rows


def attend(query_lat, query_pe, keys, visible):
    row_count, head_count, latent_width = query_lat.shape
    key_count = keys.shape[1]
    pe_width = query_pe.shape[1] // head_count
    first_dot = jnp.dot(
        query_lat.reshape(row_count * head_count, latent_width),
        keys[:latent_width],
        preferred_element_type=jnp.float32,
    )
    second_dot = jnp.dot(
        query_pe.reshape(row_count * head_count, pe_width),
        keys[latent_width:],
        preferred_element_type=jnp.float32,
    )
    scores = ((first_dot + second_dot) * (1.0 / math.sqrt(QKD))).reshape(
        row_count, head_count, key_count
    )
    scores = jnp.where(visible[:, None, :], scores, -jnp.inf)
    row_max = jnp.max(scores, axis=2)
    exponent = jnp.exp(scores - row_max[:, :, None])
    row_sum = jnp.sum(exponent, axis=2)
    weights = exponent.astype(jnp.bfloat16).reshape(row_count * head_count, key_count)
    latent = lax.dot_general(
        weights, keys[:latent_width], (((1,), (1,)), ((), ())), preferred_element_type=jnp.float32
    )
    return (row_max, row_sum, latent.reshape(row_count, head_count, latent_width))


def remote(src, dst, send, recv, target):
    return pltpu.make_async_remote_copy(
        src_ref=src,
        dst_ref=dst,
        send_sem=send,
        recv_sem=recv,
        device_id=target,
        device_id_type=pl.DeviceIdType.MESH,
    )


def place():
    ctx_count, exp_count = lax.axis_size("ctx"), lax.axis_size("exp")
    ctx, exp = lax.axis_index("ctx"), lax.axis_index("exp")
    return ctx_count // 2, exp_count, ctx, exp, ctx // 2, ctx % 2


def greet(over_exp):
    ctx_count, exp_count = lax.axis_size("ctx"), lax.axis_size("exp")
    ctx, exp = lax.axis_index("ctx"), lax.axis_index("exp")
    barrier = pltpu.get_barrier_semaphore()
    peers = [((ctx + k) % ctx_count, exp) for k in range(1, ctx_count)]
    if over_exp:
        peers += [(ctx, (exp + k) % exp_count) for k in range(1, exp_count)]
    for peer in peers:
        pl.semaphore_signal(
            barrier, inc=1, device_id=peer, device_id_type=pl.DeviceIdType.MESH
        )
    pl.semaphore_wait(barrier, len(peers))


def column_block(rows, wide, ctx, exp, width):
    if not wide:
        return rows.at[ctx, exp]
    return rows.at[exp, :, pl.ds(pl.multiple_of(ctx * width, 128), width)]


def start_gather(src, out, send, recv):
    chips, _, ctx, exp, chip, core = place()
    flights = []
    for k in range(chips):
        peer = ctx + 1 - 2 * core if k == 0 else (chip + k) % chips * 2 + core
        copy = remote(src, out.at[ctx], send.at[0, k], recv.at[0, k], (peer, exp))
        copy.start()
        flights.append(copy)
    return flights


def finish_gather(out, flights, send, recv):
    chips, _, ctx, exp, chip, core = place()
    relayed = []
    for k in range(1, chips):
        flights[k].wait_recv()
        origin = (chip + chips - k) % chips * 2 + core
        copy = remote(
            out.at[origin], out.at[origin], send.at[1, k], recv.at[1, k], (ctx + 1 - 2 * core, exp)
        )
        copy.start()
        relayed.append(copy)
    flights[0].wait_recv()
    for copy in relayed:
        copy.wait_recv()
    for copy in flights + relayed:
        copy.wait_send()


def inputs_kernel(
    cache, fresh, res, ids, cache_out, fresh_out, res_out, ids_out,
    c_send, c_recv, f_send, f_recv, r_send, r_recv, i_send, i_recv, j_send, j_recv,
):
    chips, exp_count, ctx, exp, chip, core = place()
    ctx_count = 2 * chips
    greet(True)
    id_flights = []
    for k in range(1, exp_count):
        copy = remote(
            ids, ids_out.at[ctx, exp], i_send.at[k], i_recv.at[k], (ctx, (exp + k) % exp_count)
        )
        copy.start()
        id_flights.append(copy)
    cache_flights = start_gather(cache, cache_out, c_send, c_recv)
    fresh_flights = start_gather(fresh, fresh_out, f_send, f_recv)
    res_flights = []
    for k in range(1, ctx_count):
        peer = (ctx + k) % ctx_count
        copy = remote(res.at[peer], res_out.at[ctx], r_send.at[k], r_recv.at[k], (peer, exp))
        copy.start()
        res_flights.append(copy)
    cache_out[ctx] = cache[...]
    fresh_out[ctx] = fresh[...]
    res_out[ctx] = res[ctx]
    ids_out[ctx, exp] = ids[...]
    for copy in id_flights:
        copy.wait()
    for k in range(1, ctx_count):
        copy = remote(
            ids_out.at[ctx],
            ids_out.at[ctx],
            j_send.at[k],
            j_recv.at[k],
            ((ctx + k) % ctx_count, exp),
        )
        copy.start()
        res_flights.append(copy)
    finish_gather(cache_out, cache_flights, c_send, c_recv)
    finish_gather(fresh_out, fresh_flights, f_send, f_recv)
    for copy in res_flights:
        copy.wait()


def heads_kernel(src, out, send, recv):
    _, _, ctx, _, _, _ = place()
    greet(False)
    flights = start_gather(src, out, send, recv)
    out[ctx] = src[...]
    finish_gather(out, flights, send, recv)


def hidden_kernel(
    wide, part, res, out, landed, a_send, a_recv, b_send, b_recv, x_send, x_recv, f_send, f_recv
):
    chips, exp_count, ctx, exp, chip, core = place()
    partner = ctx + 1 - 2 * core
    width = part.shape[2]
    place_of = lambda c, e: column_block(out, wide, c, e, width)
    greet(True)
    first = []
    for k in range(1, exp_count):
        peer = (exp + k) % exp_count
        copy = remote(part.at[peer], landed.at[k], a_send.at[k], a_recv.at[k], (ctx, peer))
        copy.start()
        first.append(copy)
    total = part[exp].astype(jnp.float32)
    for k in range(1, exp_count):
        first[k - 1].wait_recv()
        total = total + landed[k].astype(jnp.float32)
    own = place_of(ctx, exp)
    own[...] = (res[...].astype(jnp.float32) + total).astype(jnp.bfloat16)
    pending = []
    spread = [None]
    for k in range(1, exp_count):
        copy = remote(
            own,
            own,
            b_send.at[k],
            b_recv.at[k],
            (ctx, (exp + k) % exp_count),
        )
        copy.start()
        spread.append(copy)
    for k in range(exp_count):
        if k > 0:
            spread[k].wait_recv()
        source = (exp + exp_count - k) % exp_count
        block = place_of(ctx, source)
        row = []
        for p in range(chips):
            peer = partner if p == 0 else (chip + p) % chips * 2 + core
            copy = remote(block, block, x_send.at[p, k], x_recv.at[p, k], (peer, exp))
            copy.start()
            row.append(copy)
        pending.append(row)
    last = []
    for k in range(exp_count):
        source = (exp + exp_count - k) % exp_count
        for p in range(1, chips):
            pending[k][p].wait_recv()
            origin = (chip + chips - p) % chips * 2 + core
            block = place_of(origin, source)
            copy = remote(block, block, f_send.at[p, k], f_recv.at[p, k], (partner, exp))
            copy.start()
            last.append(copy)
    for row in pending:
        row[0].wait_recv()
    for copy in last:
        copy.wait()
    for copy in first + spread[1:] + [copy for row in pending for copy in row]:
        copy.wait_send()


def combine_kernel(
    wide, y, hid, out, pair, cross_out, cross_in, home_out, home_in, final,
    p_send, p_recv, x_send, x_recv, e_send, e_recv, o_send, o_recv,
):
    chips, exp_count, ctx, exp, chip, core = place()
    partner = ctx + 1 - 2 * core
    ctx_count, tok, width = out.shape
    part_of = lambda c, e: column_block(y, wide, c, e, width)
    greet(True)
    order = list(range(1, exp_count)) + [0]
    halves, crossing, homing = {}, {}, {}
    for k in order:
        dest = (exp + k) % exp_count
        for j in list(range(1, chips)) + [0]:
            theirs = (chip + j) % chips * 2 + 1 - core
            copy = remote(
                part_of(theirs, dest),
                pair.at[k, j],
                p_send.at[k, j],
                p_recv.at[k, j],
                (partner, exp),
            )
            copy.start()
            halves[k, j] = copy
    for k in order:
        dest = (exp + k) % exp_count
        for j in range(1, chips):
            owner = (chip + j) % chips * 2 + core
            halves[k, j].wait_recv()
            both = part_of(owner, dest)[...].astype(jnp.float32) + pair[k, j].astype(jnp.float32)
            cross_out[k, j] = both.astype(jnp.bfloat16)
            copy = remote(
                cross_out.at[k, j],
                cross_in.at[k, j],
                x_send.at[k, j],
                x_recv.at[k, j],
                (owner, exp),
            )
            copy.start()
            crossing[k, j] = copy
    total = hid[...].astype(jnp.float32)
    for k in order:
        dest = (exp + k) % exp_count
        halves[k, 0].wait_recv()
        both = part_of(ctx, dest)[...].astype(jnp.float32) + pair[k, 0].astype(jnp.float32)
        for j in range(1, chips):
            crossing[k, j].wait_recv()
            both = both + cross_in[k, j].astype(jnp.float32)
        if k == 0:
            total = total + both
        else:
            home_out[k] = both.astype(jnp.bfloat16)
            copy = remote(
                home_out.at[k], home_in.at[k], e_send.at[k], e_recv.at[k], (ctx, dest)
            )
            copy.start()
            homing[k] = copy
    for k in range(1, exp_count):
        homing[k].wait_recv()
        total = total + home_in[k].astype(jnp.float32)
    for c in range(ctx_count):
        final[c] = total[c * tok : (c + 1) * tok].astype(jnp.bfloat16)
    last = []
    for k in range(1, ctx_count):
        peer = (ctx + k) % ctx_count
        copy = remote(final.at[peer], out.at[ctx], o_send.at[k], o_recv.at[k], (peer, exp))
        copy.start()
        last.append(copy)
    out[ctx] = final[ctx]
    for copy in last:
        copy.wait()
    for copy in list(halves.values()) + list(crossing.values()) + list(homing.values()):
        copy.wait_send()


def exchange(number, kernel, shapes, scratch, *operands):
    vmem = pl.BlockSpec(memory_space=pltpu.VMEM)
    held = jax.tree.leaves(shapes) + list(operands)
    held += [s for s in scratch if s.dtype == jnp.bfloat16]
    need = sum(2 * math.prod(h.shape) * h.dtype.itemsize for h in held) + SPARE_BYTES
    return pl.pallas_call(
        kernel,
        out_shape=shapes,
        in_specs=[vmem] * len(operands),
        out_specs=jax.tree.map(lambda _: vmem, shapes),
        scratch_shapes=scratch,
        compiler_params=pltpu.CompilerParams(
            collective_id=number, has_side_effects=True, vmem_limit_bytes=min(need, VMEM_BYTES)
        ),
    )(*operands)


def staged_body(
    q_nope,
    q_rope,
    cache_keys,
    fresh_keys,
    block_order,
    w_uv,
    w_out,
    residual,
    norm_gain,
    router_weight,
    expert_ids,
    w_gate,
    w_up,
    w_down,
):
    ctx_count = lax.axis_size("ctx")
    exp_count = lax.axis_size("exp")
    ctx_index = lax.axis_index("ctx")
    exp_index = lax.axis_index("exp")
    rows_here, heads_here, latent_width = q_nope.shape
    value_width = w_uv.shape[2]
    key_width, cache_len = cache_keys.shape
    tok_here, model_width = residual.shape
    col_part = w_out.shape[1]
    chips = ctx_count // 2
    block_rows = rows_here * ctx_count // block_order.shape[0]
    dma = pltpu.SemaphoreType.DMA
    bf16 = functools.partial(jax.ShapeDtypeStruct, dtype=jnp.bfloat16)

    res_cols = residual.reshape(tok_here, ctx_count, col_part).transpose(1, 0, 2)
    cache_all, fresh_all, res_own, ids_all = exchange(
        0,
        inputs_kernel,
        (
            bf16((ctx_count, key_width, cache_len)),
            bf16((ctx_count, rows_here, key_width)),
            bf16((ctx_count, tok_here, col_part)),
            jax.ShapeDtypeStruct((ctx_count, exp_count) + expert_ids.shape, jnp.int32),
        ),
        [dma((2, chips))] * 4 + [dma((ctx_count,))] * 2 + [dma((exp_count,))] * 2
        + [dma((ctx_count,))] * 2,
        cache_keys, fresh_keys.T, res_cols, expert_ids,
    )
    cached = jnp.transpose(cache_all, (1, 0, 2)).reshape(key_width, ctx_count * cache_len)
    fresh = fresh_all.reshape(ctx_count * rows_here, key_width).T
    keys = jnp.concatenate([cached, fresh], axis=1)
    own_rows = ctx_index * rows_here + jnp.arange(rows_here, dtype=jnp.int32)
    own_pos = block_position(own_rows, block_order, block_rows)
    new_rows = jnp.arange(ctx_count * rows_here, dtype=jnp.int32)
    key_pos = jnp.concatenate(
        [
            jnp.full((ctx_count * cache_len,), -1, jnp.int32),
            block_position(new_rows, block_order, block_rows),
        ]
    )
    visible = key_pos[None, :] <= own_pos[:, None]
    row_max, row_sum, latent = attend(q_nope, q_rope, keys, visible)
    normal_lat = (latent / row_sum[:, :, None]).astype(jnp.bfloat16)
    head_out = jnp.einsum(
        "rhl,hlv->rhv", normal_lat, w_uv, preferred_element_type=jnp.float32
    ).astype(jnp.bfloat16).reshape(rows_here, heads_here * value_width)
    heads_all = exchange(
        1,
        heads_kernel,
        bf16((ctx_count,) + head_out.shape),
        [dma((2, chips))] * 2,
        head_out,
    )
    heads_all = (
        heads_all.reshape(ctx_count, exp_count, tok_here, -1)
        .transpose(1, 0, 2, 3)
        .reshape(exp_count * ctx_count * tok_here, -1)
    )
    head_partial = jnp.dot(heads_all, w_out, preferred_element_type=jnp.float32)
    group = ctx_count * tok_here
    wide = col_part % 128 == 0
    tokens = exp_count * group
    stripes = (exp_count, group, model_width)
    blocks = (ctx_count, exp_count, group, col_part)
    hidden_all = exchange(
        2,
        functools.partial(hidden_kernel, wide),
        bf16(stripes if wide else blocks),
        [pltpu.VMEM((exp_count, group, col_part), jnp.bfloat16)]
        + [dma((exp_count,))] * 4
        + [dma((chips, exp_count))] * 4,
        head_partial.astype(jnp.bfloat16).reshape(exp_count, group, col_part),
        res_own.reshape(group, col_part),
    )
    if not wide:
        hidden_all = hidden_all.transpose(1, 2, 0, 3)
    hidden_rows = hidden_all.reshape(tokens, model_width)
    hidden = hidden_rows.astype(jnp.float32)
    mean_square = jnp.mean(hidden * hidden, axis=1, keepdims=True)
    normed = (hidden * lax.rsqrt(mean_square + NORM_EPS) * norm_gain).astype(jnp.bfloat16)
    affinity = jax.nn.sigmoid(jnp.dot(normed, router_weight, preferred_element_type=jnp.float32))
    expert_count = router_weight.shape[1]
    ids = ids_all.transpose(1, 0, 2, 3).reshape(tokens, -1)
    onehot = ids[:, :, None] == jnp.arange(expert_count, dtype=jnp.int32)[None, None, :]
    named = jnp.any(onehot, axis=1)
    chosen = jnp.where(named, affinity, 0.0)
    mixing = ROUTE_SCALE * chosen / jnp.sum(chosen, axis=1, keepdims=True)
    local_experts, _, hidden_units = w_gate.shape
    mine = lax.dynamic_slice_in_dim(mixing, exp_index * local_experts, local_experts, axis=1)
    acts = []
    for i in range(local_experts):
        gate = jnp.dot(normed, w_gate[i], preferred_element_type=jnp.float32)
        upward = jnp.dot(normed, w_up[i], preferred_element_type=jnp.float32)
        acts.append((jax.nn.silu(gate) * upward * mine[:, i : i + 1]).astype(jnp.bfloat16))
    acts = jnp.concatenate(acts, axis=1)
    down = w_down.reshape(local_experts * hidden_units, model_width)
    mixed = jnp.dot(acts, down, preferred_element_type=jnp.float32).astype(jnp.bfloat16)
    own_hidden = lax.dynamic_slice(
        hidden_rows, (exp_index * group, ctx_index * col_part), (group, col_part)
    )
    mixed = mixed.reshape(stripes)
    if not wide:
        mixed = mixed.reshape(exp_count, group, ctx_count, col_part).transpose(2, 0, 1, 3)
    block = (group, col_part)
    owned = exchange(
        3,
        functools.partial(combine_kernel, wide),
        bf16((ctx_count, tok_here, col_part)),
        [pltpu.VMEM((exp_count, chips) + block, jnp.bfloat16)] * 3
        + [pltpu.VMEM((exp_count,) + block, jnp.bfloat16)] * 2
        + [pltpu.VMEM((ctx_count, tok_here, col_part), jnp.bfloat16)]
        + [dma((exp_count, chips))] * 4
        + [dma((exp_count,))] * 2
        + [dma((ctx_count,))] * 2,
        mixed,
        own_hidden,
    )
    return owned.transpose(1, 0, 2).reshape(tok_here, model_width)


GROUPS = 4
FOLD = 2


def widths(total, unit, parts):
    tiles = total // unit
    return [(tiles // parts + (1 if i < tiles % parts else 0)) * unit for i in range(parts)]


def offsets(sizes):
    return [sum(sizes[:i]) for i in range(len(sizes))]


def fits(ctx_count, exp_count, q_nope, cache_keys, w_uv, w_out, residual, w_gate, block_rows):
    rows, heads, lat = q_nope.shape
    weights = 2 * (math.prod(w_uv.shape) + math.prod(w_out.shape) + 3 * math.prod(w_gate.shape))
    return (
        ctx_count == 4
        and exp_count % FOLD == 0
        and residual.shape[0] * exp_count == rows
        and residual.shape[0] * ctx_count % 8 == 0
        and heads % GROUPS == 0
        and rows % 16 == 0
        and rows % block_rows == 0
        and w_out.shape[1] % 256 == 0
        and cache_keys.shape[1] % 128 == 0
        and lat % 128 == 0
        and w_gate.shape[2] % 128 == 0
        and weights < 54 * 1024 * 1024
        and residual.shape[1] % 1024 == 0
        and w_out.shape[1] >= 1024
        and residual.shape[1] // 1024 * rows * ctx_count <= w_out.shape[0]
    )


def quo(i, n):
    return lax.shift_right_logical(i, n.bit_length() - 1) if n & (n - 1) == 0 else i // n


def rem(i, n):
    return i & (n - 1) if n & (n - 1) == 0 else i % n


def onehot(shape, source):
    row = lax.broadcasted_iota(jnp.int32, (shape[0], 1), 0)
    col = lax.broadcasted_iota(jnp.int32, shape, 1)
    return jnp.where(col == source(row), 1.0, 0.0).astype(jnp.bfloat16)


def mm(a, b):
    return jnp.dot(a, b, preferred_element_type=jnp.float32)


def mm_t(a, b):
    return lax.dot_general(a, b, (((1,), (1,)), ((), ())), preferred_element_type=jnp.float32)


class Plan:
    rates = dict(x=46e3, y=46e3, z=35e3, d=600e3)
    delays = dict(x=2.0, y=2.0, z=2.6, d=1.1)

    def __init__(self):
        self.now, self.free, self.landed, self.tasks = 0.0, {}, {}, []

    def note(self, key, link, size):
        done = max(self.free.get(link, 0.0), self.now) + size / self.rates[link]
        self.free[link] = done
        self.landed[key] = done + self.delays[link]

    def task(self, name, run, needs=(), after=(), cost=0.05, idle=False):
        self.tasks.append((name, run, tuple(needs), tuple(after), cost, idle))

    def run(self):
        left, done, order = list(self.tasks), set(), []
        while left:
            best = None
            for rank, (name, _, needs, after, cost, idle) in enumerate(left):
                if all(a in done for a in after) and all(k in self.landed for k in needs):
                    ready = max([self.landed[k] for k in needs] + [self.now])
                    key = (ready, idle, rank)
                    if best is None or key < best:
                        best = key
            ready, _, rank = best
            name, run, _, _, cost, _ = left.pop(rank)
            self.now = ready + cost
            run()
            done.add(name)
            order.append((round(self.now, 2), name))
        self.tasks = []
        return order


def fused_kernel(
    names, dims,
    q_nope, q_rope, cache, fresh, order, w_uv, w_out, res, gain, router, ids, w_gate, w_up, w_down,
    out, *refs,
):
    s = types.SimpleNamespace(**dict(zip(names, refs)))
    d = dims
    bf16, f32 = jnp.bfloat16, jnp.float32
    ctx, exp = lax.axis_index("ctx"), lax.axis_index("exp")
    C, E, Z = d.ctx_count, d.exp_count, d.exp_count // FOLD
    x, core = ctx // 2, ctx % 2
    z, y = exp // FOLD, exp % FOLD
    xctx = (1 - x) * 2 + core
    partner = (ctx + 1 - 2 * core, exp)
    xpeer = (xctx, exp)
    ypeer = (ctx, z * FOLD + 1 - y)
    zpeer = lambda j: (ctx, (z + j) % Z * FOLD + y)
    rows, heads, lat, rope = d.rows, d.heads, d.lat, d.rope
    vals, col, tok, tokens = d.vals, d.col, d.tok, d.tokens
    group = C * tok
    hg = heads // GROUPS
    sent = []

    plan = Plan()

    def push(src, dst, sems, index, target, key=None, link=None, size=0):
        send, recv = sems
        if key is not None:
            plan.note(key, link, 2.0 * size)
        copy = remote(src, dst, send.at[index], recv.at[index], target)
        copy.start()
        sent.append(copy)
        return copy

    def load(src, dst, index):
        copy = pltpu.make_async_copy(src, dst, s.load.at[index])
        copy.start()
        return copy

    lanes = lambda start, size: pl.ds(pl.multiple_of(start, 128), size)

    l_cache = load(cache, s.kall.at[:, lanes(ctx * d.cached, d.cached)], 0)
    l_fresh = load(fresh, s.kfresh.at[pl.ds(pl.multiple_of(ctx * rows, 16), rows)], 1)
    l_res = load(res, s.res, 2)
    l_ids = load(ids, s.ids, 3)
    l_order = load(order, s.order, 4)
    l_q = load(q_nope, s.qn, 5)
    l_qr = load(q_rope, s.qr, 6)
    l_uv = load(w_uv, s.wuv, 7)
    l_gain = load(gain, s.gain, 8)
    l_router = load(router, s.router, 9)
    l_out = load(w_out, s.wout, 10)
    barrier = pltpu.get_barrier_semaphore()
    inner_left, inner_right = z > 0, z < Z - 1
    left, right = (ctx, (z - 1) * FOLD + y), (ctx, (z + 1) * FOLD + y)
    hail = functools.partial(pl.semaphore_signal, inc=1, device_id_type=pl.DeviceIdType.MESH)
    count_of = lambda a, b: a.astype(jnp.int32) + b.astype(jnp.int32)
    for k in range(1, C):
        hail(barrier, device_id=((ctx + k) % C, exp))
    hail(barrier, device_id=ypeer)
    pl.when(inner_left)(lambda: hail(barrier, device_id=left))
    pl.when(inner_right)(lambda: hail(barrier, device_id=right))
    pl.semaphore_wait(barrier, C + count_of(inner_left, inner_right))

    l_cache.wait()
    l_fresh.wait()
    key_sems = (s.k_send, s.k_recv)

    def send_keys(owner, index, target):
        a = s.kall.at[:, lanes(owner * d.cached, d.cached)]
        b = s.kfresh.at[pl.ds(pl.multiple_of(owner * rows, 16), rows)]
        return [push(a, a, key_sems, (0, index), target), push(b, b, key_sems, (1, index), target)]

    k_cross = send_keys(ctx, 0, xpeer)
    k_pair = send_keys(ctx, 1, partner)

    l_res.wait()
    r_flights = []
    for k in range(1, C):
        peer = (ctx + k) % C
        r_flights.append(
            push(s.res.at[:, lanes(peer * col, col)], s.rin.at[ctx], (s.r_send, s.r_recv), k, (peer, exp))
        )
    s.rin[ctx] = s.res[:, lanes(ctx * col, col)]
    l_ids.wait()
    named = jnp.zeros((tok, 128), f32)
    lane = lax.broadcasted_iota(jnp.int32, (tok, 128), 1)
    for k in range(d.top):
        named = named + jnp.where(s.ids[:, k : k + 1] == lane, 1.0, 0.0)
    s.nsrc[...] = jnp.zeros((8, 128), f32)
    s.nsrc[0:tok, :] = named
    s.nall[exp, ctx] = s.nsrc[...]
    for r in range(2, Z):
        tell_right = jnp.logical_and(z >= r - 1, inner_right)
        tell_left = jnp.logical_and(z <= Z - r, inner_left)
        pl.when(tell_right)(lambda r=r: hail(s.relay.at[0, r], device_id=right))
        pl.when(tell_left)(lambda r=r: hail(s.relay.at[1, r], device_id=left))
        pl.when(z >= r)(lambda r=r: pl.semaphore_wait(s.relay.at[0, r], 1))
        pl.when(z <= Z - 1 - r)(lambda r=r: pl.semaphore_wait(s.relay.at[1, r], 1))
    n_flights = [
        push(s.nsrc, s.nall.at[exp, ctx], (s.n_send, s.n_recv), k, zpeer(k)) for k in range(1, Z)
    ]

    l_q.wait()
    for g in range(GROUPS):
        part = hg * rows
        perm = onehot((part, rows * heads), lambda i: rem(i, rows) * heads + g * hg + quo(i, rows))
        s.qh[g * part : (g + 1) * part, :] = mm(perm, s.qn[...]).astype(bf16)
    l_qr.wait()
    for h in range(heads):
        s.qrh[h * rows : (h + 1) * rows, :] = s.qr[:, h * rope : (h + 1) * rope]

    l_order.wait()
    size = d.block
    own_blocks = rows // size
    part = hg * rows
    row_id = rem(lax.broadcasted_iota(jnp.int32, (part, 1), 0), rows)
    key_id = lax.broadcasted_iota(jnp.int32, (1, tokens), 1)
    own_pos = rem(row_id, size)
    key_pos = rem(key_id, size)
    for b in range(own_blocks):
        own_pos = own_pos + jnp.where(quo(row_id, size) == b, s.order[ctx * own_blocks + b] * size, 0)
    for b in range(tokens // size):
        key_pos = key_pos + jnp.where(quo(key_id, size) == b, s.order[b] * size, 0)
    s.bias[...] = jnp.where(key_pos <= own_pos, 0.0, -jnp.inf)
    l_uv.wait()
    l_gain.wait()
    l_router.wait()
    l_out.wait()
    l_gate = load(w_gate, s.wg, 11)
    l_up = load(w_up, s.wu, 12)
    l_down = load(w_down, s.wd, 13)

    for copy in k_cross:
        copy.wait_recv()
    k_far = send_keys(xctx, 2, partner)
    for copy in k_pair + k_far:
        copy.wait_recv()

    scale = 1.0 / math.sqrt(QKD)
    h_cross, h_pair = [], []
    for g in range(GROUPS):
        q = s.qh[g * part : (g + 1) * part, :]
        qr = s.qrh[g * part : (g + 1) * part, :]
        old = (mm(q, s.kall[0:lat, :]) + mm(qr, s.kall[lat : lat + rope, :])) * scale
        new = (mm_t(q, s.kfresh[:, 0:lat]) + mm_t(qr, s.kfresh[:, lat : lat + rope])) * scale
        new = new + s.bias[...]
        top = jnp.maximum(jnp.max(old, axis=1, keepdims=True), jnp.max(new, axis=1, keepdims=True))
        old = jnp.exp(old - top)
        new = jnp.exp(new - top)
        total = jnp.sum(old, axis=1, keepdims=True) + jnp.sum(new, axis=1, keepdims=True)
        latent = mm_t(old.astype(bf16), s.kall[0:lat, :]) + mm(new.astype(bf16), s.kfresh[:, 0:lat])
        latent = (latent / total).astype(bf16)
        for h in range(hg):
            one = mm(latent[h * rows : (h + 1) * rows], s.wuv[g * hg + h])
            s.heads[ctx, g, :, h * vals : (h + 1) * vals] = one.astype(bf16)
        view = s.heads.at[ctx, g]
        h_cross.append(push(view, view, (s.h_send, s.h_recv), (0, g), xpeer))
        h_pair.append(push(view, view, (s.h_send, s.h_recv), (1, g), partner))
    for copy in n_flights:
        copy.wait_recv()
    named_y = []
    for j in range(Z):
        view = s.nall.at[(z + Z - j) % Z * FOLD + y, ctx]
        named_y.append(push(view, view, (s.o_send, s.o_recv), j, ypeer))
    h_far = []
    for g in range(GROUPS):
        h_cross[g].wait_recv()
        view = s.heads.at[xctx, g]
        h_far.append(push(view, view, (s.h_send, s.h_recv), (2, g), partner))

    deep = hg * vals
    for g in range(GROUPS - 1):
        h_pair[g].wait_recv()
        h_far[g].wait_recv()
        value = mm(s.heads[:, g].reshape(tokens, deep), s.wout[g * deep : (g + 1) * deep, :])
        s.pacc[...] = value if g == 0 else s.pacc[...] + value
    h_pair[GROUPS - 1].wait_recv()
    h_far[GROUPS - 1].wait_recv()

    for copy in named_y:
        copy.wait_recv()
    n_last = []
    for k in range(1, C):
        view = s.nall.at[:, ctx]
        n_last.append(push(view, view, (s.m_send, s.m_recv), k, ((ctx + k) % C, exp)))

    chunks = d.chunks
    starts = offsets(chunks)
    to_group = onehot(
        (tokens, tokens), lambda i: rem(quo(i, tok), C) * rows + quo(i, group) * tok + rem(i, tok)
    )
    flights = {}
    count = len(chunks)
    ahead = d.ahead

    def open_sum(q):
        o, w = starts[q], chunks[q]
        value = s.pacc[:, o : o + w] + mm(
            s.heads[:, GROUPS - 1].reshape(tokens, deep), s.wout[(GROUPS - 1) * deep :, o : o + w]
        )
        value = mm(to_group, value.astype(bf16)).astype(bf16)
        s.p[:, :, :, o : o + w] = value.reshape(Z, FOLD, group, w)
        flights["y", q] = push(
            s.p.at[:, 1 - y, :, pl.ds(o, w)], s.yin.at[:, :, pl.ds(o, w)],
            (s.y_send, s.y_recv), q, ypeer, ("y", q), "y", Z * group * w,
        )

    def sum_y(q):
        o, w = starts[q], chunks[q]
        flights["y", q].wait_recv()
        both = s.p[:, y, :, o : o + w].astype(f32) + s.yin[:, :, o : o + w].astype(f32)
        s.zsrc[:, :, o : o + w] = both.astype(bf16)
        for j in range(1, Z):
            flights["z", q, j] = push(
                s.zsrc.at[(z + j) % Z, :, pl.ds(o, w)], s.zin.at[j, :, pl.ds(o, w)],
                (s.z_send, s.z_recv), (q, j), zpeer(j), ("z", q, j), "z", group * w,
            )

    def add_residual():
        for copy in r_flights:
            copy.wait_recv()
        for c in range(C):
            s.rsum[c * tok : (c + 1) * tok, :] = s.rin[c].astype(f32)

    def block(c, e, q):
        return s.hid.at[e, :, lanes(c * col + starts[q], chunks[q])]

    def spread(q, step, index, c, e, target):
        view = block(c, e, q)
        link = step if step in "zd" else ("y" if (step == "a") == ahead[q] else "x")
        flights["g" + step, q, index] = push(
            view, view, (s.g_send, s.g_recv), (q, d.slot[step, index]), target,
            ("g" + step, q, index), link, group * chunks[q],
        )

    def axes(q):
        return (ypeer, xpeer) if ahead[q] else (xpeer, ypeer)

    def near(q, j):
        return ctx, (z + Z - j) % Z * FOLD + y

    def first(q, j):
        c, e = near(q, j)
        return (c, e + 1 - 2 * y) if ahead[q] else (xctx, e)

    def second(q, i):
        c, e = near(q, i) if i < Z else first(q, i - Z)
        return (xctx, e) if ahead[q] else (c, e + 1 - 2 * y)

    def sum_z(q):
        o, w = starts[q], chunks[q]
        both = s.p[z, y, :, o : o + w].astype(f32) + s.yin[z, :, o : o + w].astype(f32)
        for j in range(1, Z):
            flights["z", q, j].wait_recv()
            both = both + s.zin[j, :, o : o + w].astype(f32)
        both = both + s.rsum[:, o : o + w]
        s.hid[exp, :, lanes(ctx * col + o, w)] = both.astype(bf16)
        c, e = near(q, 0)
        a, b = axes(q)
        for j in range(1, Z):
            spread(q, "z", j, c, e, zpeer(j))
        spread(q, "a", 0, c, e, a)
        spread(q, "b", 0, c, e, b)
        spread(q, "d", 0, c, e, partner)

    def pass_near(q, j):
        a, b = axes(q)
        flights["gz", q, j].wait_recv()
        c, e = near(q, j)
        spread(q, "a", j, c, e, a)
        spread(q, "b", j, c, e, b)
        spread(q, "d", j, c, e, partner)

    def pass_first(q, j):
        _, b = axes(q)
        flights["ga", q, j].wait_recv()
        c, e = first(q, j)
        spread(q, "b", Z + j, c, e, b)
        spread(q, "d", Z + j, c, e, partner)

    def pass_second(q, i):
        flights["gb", q, i].wait_recv()
        c, e = second(q, i)
        spread(q, "d", 2 * Z + i, c, e, partner)

    units = d.units

    def open_units():
        l_gate.wait()
        l_up.wait()
        s.ss[...] = jnp.zeros(s.ss.shape, f32)
        s.racc[...] = jnp.zeros(s.racc.shape, f32)
        s.gacc[...] = jnp.zeros(s.gacc.shape, f32)
        s.uacc[...] = jnp.zeros(s.uacc.shape, f32)

    def consume(q, c, arrivals):
        for key in arrivals:
            flights[key].wait_recv()
        w = chunks[q]
        at = lanes(c * col + starts[q], w)
        hidden = s.hid[:, :, at].reshape(tokens, w).astype(f32)
        square = hidden * hidden
        some = square[:, 0:128]
        for k in range(1, w // 128):
            some = some + square[:, k * 128 : (k + 1) * 128]
        s.ss[...] = s.ss[...] + some
        scaled = (hidden * s.gain[:, at]).astype(bf16)
        s.racc[...] = s.racc[...] + mm_t(scaled, s.router[:, at])
        for k in range(d.local):
            here = slice(k * units, (k + 1) * units)
            s.gacc[:, here] = s.gacc[:, here] + mm(scaled, s.wg[k, at, :])
            s.uacc[:, here] = s.uacc[:, here] + mm(scaled, s.wu[k, at, :])

    call = functools.partial
    plan.task("residual", add_residual, cost=0.3)
    for q in range(count):
        w = chunks[q] / 512
        plan.task(("o", q), call(open_sum, q), after=[("o", q - 1)] if q else [], cost=0.15 * w)
    plan.task("units", open_units, cost=0.3, idle=True)
    for q in range(count):
        w = chunks[q] / 512
        plan.task(("sy", q), call(sum_y, q), [("y", q)], cost=0.2 * w)
        plan.task(
            ("sz", q), call(sum_z, q), [("z", q, j) for j in range(1, Z)],
            ["residual", ("sy", q)], cost=0.15 * w,
        )
        for j in range(1, Z):
            plan.task(("n", q, j), call(pass_near, q, j), [("gz", q, j)], [("sz", q)])
        for j in range(Z):
            plan.task(("f", q, j), call(pass_first, q, j), [("ga", q, j)], [("sz", q)])
        for i in range(2 * Z):
            plan.task(("s", q, i), call(pass_second, q, i), [("gb", q, i)], [("sz", q)])
        nears = [("sz", q)] + [("n", q, j) for j in range(1, Z)]
        firsts = [("f", q, j) for j in range(Z)]
        seconds = [("s", q, i) for i in range(2 * Z)]
        if ahead[q]:
            mine, theirs = nears + firsts, seconds
            own_d = list(range(2 * Z))
        else:
            mine, theirs = nears + seconds[:Z], firsts + seconds[Z:]
            own_d = list(range(Z)) + list(range(2 * Z, 3 * Z))
        far_d = [i for i in range(4 * Z) if i not in own_d]
        pair_c, far_c = ctx + 1 - 2 * core, xctx + 1 - 2 * core
        near_keys, far_keys = [("gd", q, i) for i in own_d], [("gd", q, i) for i in far_d]
        late = dict(cost=0.4 * w, idle=True)
        plan.task(("c", q, 0), call(consume, q, ctx, []), [], mine + ["units"], **late)
        plan.task(("c", q, 1), call(consume, q, pair_c, near_keys), near_keys, ["units"], **late)
        plan.task(("c", q, 2), call(consume, q, xctx, []), [], theirs + ["units"], **late)
        plan.task(("c", q, 3), call(consume, q, far_c, far_keys), far_keys, ["units"], **late)
    trail = plan.run()

    for copy in n_last:
        copy.wait_recv()
    squeeze = onehot((tokens, tokens // tok * 8), lambda i: quo(i, tok) * 8 + rem(i, tok))
    named = mm(squeeze, s.nall[...].reshape(tokens // tok * 8, 128).astype(bf16))
    named = named[:, 0 : d.experts]
    mean = jnp.sum(s.ss[...], axis=1, keepdims=True) * (1.0 / d.width)
    factor = lax.rsqrt(mean + NORM_EPS)
    affinity = jax.nn.sigmoid(s.racc[...] * factor)
    chosen = jnp.where(named > 0.5, affinity, 0.0)
    mixing = ROUTE_SCALE * chosen / jnp.sum(chosen, axis=1, keepdims=True)
    which = lax.broadcasted_iota(jnp.int32, (tokens, d.experts), 1)
    for k in range(d.local):
        here = slice(k * units, (k + 1) * units)
        mine = jnp.sum(jnp.where(which == exp * d.local + k, mixing, 0.0), axis=1, keepdims=True)
        gate = s.gacc[:, here] * factor
        upward = s.uacc[:, here] * factor
        s.acts[:, here] = (gate * jax.nn.sigmoid(gate) * upward * mine).astype(bf16)

    def owner_order(i):
        t, zz, yy = rem(i, tok), rem(quo(i, tok), Z), rem(quo(i, tok * Z), FOLD)
        xx, kk = rem(quo(i, tok * Z * FOLD), 2), quo(i, tok * Z * FOLD * 2)
        return (zz * FOLD + yy) * group + (xx * 2 + kk) * tok + t

    to_owner = onehot((tokens, tokens), owner_order)
    for k in range(d.local):
        here = slice(k * units, (k + 1) * units)
        s.acts[:, here] = mm(to_owner, s.acts[:, here]).astype(bf16)
    l_down.wait()
    cw, n = d.out_width, d.width // d.out_width
    half, quarter, eighth = tokens // 2, tokens // 4, tokens // 8
    pairs, hops, lasts, ends = {}, {}, {}, {}

    def produce(i):
        mixed = mm(s.acts[...], s.wd[:, i * cw : (i + 1) * cw]).astype(bf16)
        s.wout[i * tokens : (i + 1) * tokens, 0:cw] = mixed
        away = s.wout.at[pl.ds(pl.multiple_of(i * tokens + (1 - core) * half, 16), half), pl.ds(0, cw)]
        pairs[i] = push(away, s.pair.at[i], (s.p_send, s.p_recv), i, partner, ("p", i), "d", half * cw)

    def join_pair(i):
        pairs[i].wait_recv()
        mine = s.wout[pl.ds(pl.multiple_of(i * tokens + core * half, 16), half), 0:cw]
        both = mine.astype(f32) + s.pair[i].astype(f32)
        s.s1[i] = both.astype(bf16).reshape(2, FOLD, eighth, cw)
        if i % 2 == 0:
            hops[i] = push(
                s.s1.at[i, 1 - x], s.h1.at[i], (s.a_send, s.a_recv), i, xpeer,
                ("a", i), "x", quarter * cw,
            )
        else:
            hops[i] = push(
                s.s1.at[i, :, 1 - y], s.h1.at[i], (s.a_send, s.a_recv), i, ypeer,
                ("a", i), "y", quarter * cw,
            )

    def join_hop(i):
        hops[i].wait_recv()
        mine = s.s1[i, x] if i % 2 == 0 else s.s1[i, :, y]
        s.s2[i] = (mine.astype(f32) + s.h1[i].astype(f32)).astype(bf16)
        if i % 2 == 0:
            lasts[i] = push(
                s.s2.at[i, 1 - y], s.h2.at[i], (s.b_send, s.b_recv), i, ypeer,
                ("b", i), "y", eighth * cw,
            )
        else:
            lasts[i] = push(
                s.s2.at[i, 1 - x], s.h2.at[i], (s.b_send, s.b_recv), i, xpeer,
                ("b", i), "x", eighth * cw,
            )

    def join_last(i):
        lasts[i].wait_recv()
        mine = s.s2[i, y] if i % 2 == 0 else s.s2[i, x]
        s.total[...] = mine.astype(f32) + s.h2[i].astype(f32)
        for zz in range(Z):
            s.zo[i, zz] = s.total[zz * tok : (zz + 1) * tok, :].astype(bf16)
        ends[i] = [
            push(
                s.zo.at[i, (z + j) % Z], s.zi.at[i, j], (s.e_send, s.e_recv), (i, j), zpeer(j),
                ("e", i, j), "z", tok * cw,
            )
            for j in range(1, Z)
        ]

    def finish(i):
        at = slice(i * cw, (i + 1) * cw)
        s.total[...] = s.hid[exp, :, at].astype(f32)
        value = s.zo[i, z].astype(f32)
        for c in range(C):
            value = value + jnp.where(ctx == c, s.total[c * tok : (c + 1) * tok, :], 0.0)
        for j in range(1, Z):
            ends[i][j - 1].wait_recv()
            value = value + s.zi[i, j].astype(f32)
        out[:, at] = value.astype(bf16)

    for i in range(n):
        plan.task(("o", i), call(produce, i), after=[("o", i - 1)] if i else [], cost=0.35, idle=True)
        plan.task(("p", i), call(join_pair, i), [("p", i)], cost=0.25)
        plan.task(("a", i), call(join_hop, i), [("a", i)], cost=0.15)
        plan.task(("b", i), call(join_last, i), [("b", i)], cost=0.1)
        plan.task(("e", i), call(finish, i), [("e", i, j) for j in range(1, Z)], cost=0.05)
    trail = trail + plan.run()

    for copy in sent:
        copy.wait_send()


def fused_body(dims, arguments):
    (
        q_nope, q_rope, cache_keys, fresh_keys, block_order, w_uv, w_out, residual, norm_gain,
        router_weight, expert_ids, w_gate, w_up, w_down,
    ) = arguments
    d = dims
    bf16, f32 = jnp.bfloat16, jnp.float32
    dma = pltpu.SemaphoreType.DMA
    vmem = pltpu.VMEM
    C, E, Z, Y = d.ctx_count, d.exp_count, d.exp_count // FOLD, FOLD
    group = C * d.tok
    keys = d.lat + d.rope
    n = d.width // d.out_width
    queries = d.rows * d.heads
    part = queries // GROUPS
    hidden = d.local * d.units
    q = len(d.chunks)
    scratch = dict(
        wuv=vmem(w_uv.shape, bf16),
        wout=vmem(w_out.shape, bf16),
        wg=vmem(w_gate.shape, bf16),
        wu=vmem(w_up.shape, bf16),
        wd=vmem((hidden, d.width), bf16),
        qn=vmem((queries, d.lat), bf16),
        qh=vmem((queries, d.lat), bf16),
        qr=vmem(q_rope.shape, bf16),
        qrh=vmem((queries, d.rope), bf16),
        kall=vmem((keys, C * d.cached), bf16),
        kfresh=vmem((d.tokens, keys), bf16),
        bias=vmem((part, d.tokens), f32),
        res=vmem(residual.shape, bf16),
        rin=vmem((C, d.tok, d.col), bf16),
        rsum=vmem((group, d.col), f32),
        ids=vmem(expert_ids.shape, jnp.int32),
        nsrc=vmem((8, 128), f32),
        nall=vmem((E, C, 8, 128), f32),
        order=pltpu.SMEM(block_order.shape, jnp.int32),
        gain=vmem((1, d.width), f32),
        router=vmem((d.experts, d.width), bf16),
        heads=vmem((C, GROUPS, d.rows, d.heads // GROUPS * d.vals), bf16),
        pacc=vmem((d.tokens, d.col), f32),
        p=vmem((Z, Y, group, d.col), bf16),
        yin=vmem((Z, group, d.col), bf16),
        zsrc=vmem((Z, group, d.col), bf16),
        zin=vmem((Z, group, d.col), bf16),
        hid=vmem((E, group, d.width), bf16),
        ss=vmem((d.tokens, 128), f32),
        racc=vmem((d.tokens, d.experts), f32),
        gacc=vmem((d.tokens, hidden), f32),
        uacc=vmem((d.tokens, hidden), f32),
        acts=vmem((d.tokens, hidden), bf16),
        pair=vmem((n, d.tokens // 2, d.out_width), bf16),
        s1=vmem((n, 2, Y, d.tokens // 8, d.out_width), bf16),
        h1=vmem((n, 2, d.tokens // 8, d.out_width), bf16),
        s2=vmem((n, 2, d.tokens // 8, d.out_width), bf16),
        h2=vmem((n, d.tokens // 8, d.out_width), bf16),
        total=vmem((d.tokens // 8, d.out_width), f32),
        zo=vmem((n, Z, d.tok, d.out_width), bf16),
        zi=vmem((n, Z, d.tok, d.out_width), bf16),
        load=dma((14,)),
        k_send=dma((2, 3)), k_recv=dma((2, 3)),
        r_send=dma((C,)), r_recv=dma((C,)),
        n_send=dma((Z,)), n_recv=dma((Z,)),
        o_send=dma((Z,)), o_recv=dma((Z,)),
        relay=pltpu.SemaphoreType.REGULAR((2, Z)),
        m_send=dma((C,)), m_recv=dma((C,)),
        h_send=dma((3, GROUPS)), h_recv=dma((3, GROUPS)),
        y_send=dma((q,)), y_recv=dma((q,)),
        z_send=dma((q, Z)), z_recv=dma((q, Z)),
        g_send=dma((q, len(d.slot))), g_recv=dma((q, len(d.slot))),
        p_send=dma((n,)), p_recv=dma((n,)),
        a_send=dma((n,)), a_recv=dma((n,)),
        b_send=dma((n,)), b_recv=dma((n,)),
        e_send=dma((n, Z)), e_recv=dma((n, Z)),
    )
    held = SPARE_BYTES // 2 + sum(
        math.prod(k.shape[:-2]) * -(-k.shape[-2] // 8) * 8 * -(-k.shape[-1] // 128) * 128
        * jnp.dtype(k.dtype).itemsize
        for name, k in scratch.items()
        if name != "order" and not name.endswith(("load", "_send", "_recv", "relay"))
    )
    anywhere = pl.BlockSpec(memory_space=pl.ANY)
    operands = (
        q_nope.reshape(queries, d.lat), q_rope, cache_keys, fresh_keys.T, block_order, w_uv, w_out,
        residual, norm_gain.reshape(1, -1), router_weight.T, expert_ids, w_gate, w_up,
        w_down.reshape(hidden, d.width),
    )
    return pl.pallas_call(
        functools.partial(fused_kernel, tuple(scratch), d),
        out_shape=jax.ShapeDtypeStruct(residual.shape, bf16),
        in_specs=[anywhere] * len(operands),
        out_specs=pl.BlockSpec(memory_space=pltpu.VMEM),
        scratch_shapes=list(scratch.values()),
        compiler_params=pltpu.CompilerParams(
            collective_id=0, has_side_effects=True, vmem_limit_bytes=min(held, 67043328)
        ),
    )(*operands)


def body(*arguments):
    (
        q_nope, q_rope, cache_keys, _, block_order, w_uv, w_out, residual, _, router_weight,
        expert_ids, w_gate, _, _,
    ) = arguments
    ctx_count, exp_count = lax.axis_size("ctx"), lax.axis_size("exp")
    rows, heads, lat = q_nope.shape
    tokens = rows * ctx_count
    block = tokens // block_order.shape[0]
    if not fits(ctx_count, exp_count, q_nope, cache_keys, w_uv, w_out, residual, w_gate, block):
        return staged_body(*arguments)
    depth = exp_count // FOLD
    steps = [("z", j) for j in range(1, depth)] + [("a", j) for j in range(depth)]
    steps += [("b", j) for j in range(2 * depth)] + [("d", j) for j in range(4 * depth)]
    width = residual.shape[1]
    dims = types.SimpleNamespace(
        ctx_count=ctx_count, exp_count=exp_count, rows=rows, heads=heads, lat=lat,
        rope=q_rope.shape[1] // heads, vals=w_uv.shape[2], col=w_out.shape[1],
        tok=residual.shape[0], tokens=tokens, cached=cache_keys.shape[1], top=expert_ids.shape[1],
        block=block, experts=router_weight.shape[1], local=w_gate.shape[0], units=w_gate.shape[2],
        width=width, chunks=widths(w_out.shape[1], 256, 4), ahead=[True, False] * 2,
        out_width=1024,
        slot={step: i for i, step in enumerate(steps)},
    )
    return fused_body(dims, arguments)


def solution(mesh):
    return jax.shard_map(
        body,
        mesh=mesh,
        in_specs=(
            P("ctx", "exp", None),
            P("ctx", "exp"),
            P(None, "ctx"),
            P(None, "ctx"),
            P(),
            P("exp", None, None),
            P("exp", "ctx"),
            P(("ctx", "exp"), None),
            P(),
            P(),
            P(("ctx", "exp"), None),
            P("exp", None, "ctx"),
            P("exp", None, "ctx"),
            P("exp", "ctx", None),
        ),
        out_specs=P(("ctx", "exp"), None),
        check_vma=False,
    )
```
